32 devices in a mesh: groups: 1, row: 16 (over z, y, x), col: 2 (over core).
Axes of the slice: x: 2, y: 2, z: 4, core: 2. Of those that a mesh axis runs over, the one named last changes fastest.
Arguments:
- wave_now: float32 [2, 2048, 4096], P('groups', 'row', 'col'), may hold values from -6 to 6
- wave_before: float32 [2, 2048, 4096], P('groups', 'row', 'col'), may hold values from -6 to 6
- fault_slip: float32 [2048, 4096], P(('groups', 'row'), 'col'), may hold values from 0 to 2
- region_ids: int32 [128, 256], P(('groups', 'row'), 'col'), may hold values from 0 to 7
- mode_history: bfloat16 [16, 2, 4096, 2048], P('groups', None, ('row', 'col')), may hold values from -6 to 6
- wave_kernel: bfloat16 [16, 4096, 2048], P(None, ('row', 'col')), may hold values from -1.5 to 1.5
- static_friction: float32 [8], replicated, may hold values from 0.55 to 0.75
- dynamic_friction: float32 [8], replicated, may hold values from 0.2 to 0.45
- weakening_slip: float32 [8], replicated, may hold values from 0.3 to 3
- normal_stress: float32 [8], replicated, may hold values from 2 to 5
- initial_stress: float32 [8], replicated, may hold values from -1.5 to 1.5
Outputs:
- final_wave: float32 [2, 2048, 4096], P('groups', 'row', 'col')
- final_slip: float32 [2048, 4096], P(('groups', 'row'), 'col')
- fault_traction: float32 [2048, 4096], P(('groups', 'row'), 'col')
The draws below stay inside these ranges and needn't reach their ends.
All inputs are finite; a program needn't handle non-finite values.
Results may differ from the reference program's by a relative error of at most 0.0003.
Values sent between devices are 32-bit elements; how exact they have to be, the bound alone decides.
No kernel may reach another device: no remote copies, remote signals or barrier semaphores. Data moves between devices by JAX's collectives and lax.ppermute only.
A program may use at most 128 MiB of HBM per device.

```python
import math
import jax
import jax.numpy as jnp

NX = 2048
NY = 4096
DEPTH = 2
HORIZON = 16
SUBSTEPS = 2
BLOCK_CELLS = 16
REGIONS = 8
REGION_ROWS = 128
REGION_COLS = 256


def place_ends(result, key, low, top_value):
    place = [jax.random.randint(jax.random.fold_in(key, axis), (), 0, length) for axis, length in enumerate(result.shape)]
    widest = result.shape.index(max(result.shape))
    beside = place[:widest] + [(place[widest] + 1) % result.shape[widest]] + place[widest + 1:]
    return result.at[tuple(place)].set(low).at[tuple(beside)].set(top_value)


def level_of(rng, extent, split, least, largest):
    def one(axis_at, parts):
        draws = jax.random.uniform(jax.random.fold_in(jax.random.fold_in(rng, 6), axis_at), (parts,), jnp.float32, least / len(split), largest / len(split))
        return jnp.repeat(jnp.exp(draws), extent[axis_at] // parts).reshape((-1,) + (1,) * (len(extent) - axis_at - 1))

    factor_of = one(*split[0])
    for cut in split[1:]:
        factor_of = factor_of * one(*cut)
    return factor_of


def normal_values(own_key, extent, scale, reach, split=(), held_as=jnp.bfloat16):
    values = scale * jax.random.normal(own_key, extent, jnp.float32)
    if split:
        values = values * level_of(own_key, extent, split, -0.22, 0.18)
    return jnp.clip(values, -reach, reach).astype(held_as)


def setup_inputs(seed: int = 0, part: int = 0) -> dict:
    key_list = jax.random.split(jax.random.key(seed), 12)
    part_splits = jax.random.split(jax.random.fold_in(key_list[11], part), 12)
    wave_now = normal_values(part_splits[0], (DEPTH, NX, NY), 1.0, 6.0, ((1, 16), (2, 2)), jnp.float32)
    wave_before = normal_values(part_splits[1], (DEPTH, NX, NY), 1.0, 6.0, ((1, 16), (2, 2)), jnp.float32)
    fault_slip = jnp.clip(2.0 * jax.random.uniform(part_splits[2], (NX, NY), jnp.float32) ** level_of(part_splits[2], (NX, NY), ((0, 16), (1, 2)), -0.2, 0.2), 0.0, 2.0)
    region_ids = place_ends(jax.random.randint(part_splits[3], (REGION_ROWS, REGION_COLS), 0, REGIONS), jax.random.fold_in(part_splits[3], 1), 0, REGIONS - 1).astype(jnp.int32)
    mode_history = normal_values(part_splits[4], (HORIZON, 2, NY, NX), 1.0, 6.0, ((2, 32),))
    wave_kernel = normal_values(key_list[5], (HORIZON, NY, NX), 0.25, 1.5, ((1, 32),))
    static_friction = jnp.clip(jax.random.uniform(key_list[6], (REGIONS,), jnp.float32, 0.55, 0.75), 0.55, 0.75)
    dynamic_friction = jnp.clip(jax.random.uniform(key_list[7], (REGIONS,), jnp.float32, 0.2, 0.45), 0.2, 0.45)
    weakening_slip = jnp.clip(jnp.exp(jax.random.uniform(key_list[8], (REGIONS,), jnp.float32, math.log(0.3), math.log(3.0))), 0.3, 3.0)
    normal_stress = jnp.clip(jax.random.uniform(key_list[9], (REGIONS,), jnp.float32, 2.0, 5.0), 2.0, 5.0)
    initial_stress = jnp.clip(jax.random.uniform(key_list[10], (REGIONS,), jnp.float32, -1.5, 1.5), -1.5, 1.5)
    return dict(wave_now=wave_now, wave_before=wave_before, fault_slip=fault_slip, region_ids=region_ids, mode_history=mode_history, wave_kernel=wave_kernel, static_friction=static_friction, dynamic_friction=dynamic_friction, weakening_slip=weakening_slip, normal_stress=normal_stress, initial_stress=initial_stress)


damping = 0.5
courant = 0.3


def reference(wave_now, wave_before, fault_slip, region_ids, mode_history, wave_kernel, static_friction, dynamic_friction, weakening_slip, normal_stress, initial_stress):
    cell_ids = jnp.repeat(jnp.repeat(region_ids, BLOCK_CELLS, axis=0), BLOCK_CELLS, axis=1).astype(jnp.int32)
    static_level = static_friction[cell_ids]
    dynamic_level = dynamic_friction[cell_ids]
    weakening = weakening_slip[cell_ids]
    normal_load = normal_stress[cell_ids]
    prestress = initial_stress[cell_ids]
    current = wave_now
    previous = wave_before
    slip = fault_slip
    traction = jnp.zeros_like(fault_slip)
    recent = []
    for substep in range(SUBSTEPS):
        slip_rate = current[0] - previous[0]
        transform = jnp.fft.fft2(slip_rate, norm="ortho").T
        recent.insert(0, jnp.stack([jnp.real(transform), jnp.imag(transform)]).astype(jnp.float32))
        fresh = len(recent)
        wave_load = jnp.zeros((2, NY, NX), jnp.float32)
        for offset in range(fresh):
            wave_load = wave_load + wave_kernel[offset].astype(jnp.float32)[None] * recent[offset]
        for offset in range(fresh, HORIZON):
            wave_load = wave_load + wave_kernel[offset].astype(jnp.float32)[None] * mode_history[offset - fresh].astype(jnp.float32)
        combined = (wave_load[0] + 1j * wave_load[1]).T
        far_field = jnp.real(jnp.fft.ifft2(combined, norm="ortho")).astype(jnp.float32)
        trial_stress = prestress + far_field - damping * slip_rate
        strength = normal_load * (static_level - (static_level - dynamic_level) * jnp.minimum(slip / weakening, 1.0))
        traction = jnp.clip(trial_stress, -strength, strength)
        slip = slip + jnp.abs(slip_rate)
        laplacian = (jnp.roll(current, 1, 1) + jnp.roll(current, -1, 1) + jnp.roll(current, 1, 2) + jnp.roll(current, -1, 2) - 4.0 * current)
        upper_cells = jnp.concatenate([current[1:], jnp.zeros_like(current[:1])], 0)
        lower_cells = jnp.concatenate([(current[0] + traction)[None], current[:-1]], 0)
        following = 2.0 * current - previous + courant * (laplacian + upper_cells + lower_cells - 2.0 * current)
        previous = current
        current = following
    return current, slip, traction
```

```python
import functools
import math

import jax
import jax.numpy as jnp
import numpy as np
from jax import lax
from jax.experimental import pallas as pl
from jax.experimental.pallas import tpu as pltpu
from jax.sharding import PartitionSpec as P

SUBSTEPS = 2
BLOCK_CELLS = 16
LANES = 128
SUB = 8

damping = 0.5
courant = 0.3
f32 = jnp.float32
bf16 = jnp.bfloat16


def add(a, b):
    if a is None:
        return b
    return a if b is None else a + b


def sub(a, b):
    if b is None:
        return a
    return -b if a is None else a - b


def scale(z, w):
    re, im = z
    c, s = w.real, w.imag
    if abs(s) < 1e-12:
        return (re, im) if c > 0 else (-re, None if im is None else -im)
    if abs(c) < 1e-12:
        if s > 0:
            return (None if im is None else -im, re)
        return (im, None if re is None else -re)
    if im is None:
        return (re * c, re * s)
    if re is None:
        return (im * -s, im * c)
    if abs(abs(c) - abs(s)) < 1e-12:
        a = abs(c)
        signs = (c > 0, s > 0)
        if signs == (True, True):
            return ((re - im) * a, (re + im) * a)
        if signs == (True, False):
            return ((re + im) * a, (im - re) * a)
        if signs == (False, True):
            return ((re + im) * -a, (re - im) * a)
        return ((im - re) * a, (re + im) * -a)
    return (re * c - im * s, re * s + im * c)


def cadd(a, b):
    return (add(a[0], b[0]), add(a[1], b[1]))


def csub(a, b):
    return (sub(a[0], b[0]), sub(a[1], b[1]))


def conj(a):
    return (a[0], None if a[1] is None else -a[1])


def root(k, n, sign):
    return complex(math.cos(2 * math.pi * k / n), sign * math.sin(2 * math.pi * k / n))


def fft_list(zs, sign):
    n = len(zs)
    if n == 1:
        return list(zs)
    even = fft_list(zs[0::2], sign)
    odd = fft_list(zs[1::2], sign)
    low, high = [], []
    for k in range(n // 2):
        t = scale(odd[k], root(k, n, sign))
        low.append(cadd(even[k], t))
        high.append(csub(even[k], t))
    return low + high


def rfft_list(xs):
    n = len(xs)
    if n == 1:
        return [(xs[0], None)]
    if n == 2:
        return [(xs[0] + xs[1], None), (xs[0] - xs[1], None)]
    even = rfft_list(xs[0::2])
    odd = rfft_list(xs[1::2])
    out = [None] * (n // 2 + 1)
    for k in range(n // 4 + 1):
        t = scale(odd[k], root(k, n, -1.0))
        out[k] = cadd(even[k], t)
        if n // 2 - k != k:
            out[n // 2 - k] = conj(csub(even[k], t))
    return out


def irfft_list(ps):
    n = 2 * (len(ps) - 1)
    if n == 2:
        return [ps[0][0] + ps[1][0], ps[0][0] - ps[1][0]]
    even, odd = [], []
    for k in range(n // 4 + 1):
        mirrored = conj(ps[n // 2 - k])
        even.append(cadd(ps[k], mirrored))
        odd.append(scale(csub(ps[k], mirrored), root(k, n, 1.0)))
    a, b = irfft_list(even), irfft_list(odd)
    return [v for pair in zip(a, b) for v in pair]


def halves(table):
    high = table.astype(np.float32).astype(bf16)
    low = (table - high.astype(np.float64)).astype(np.float32).astype(bf16)
    return jnp.asarray(high), jnp.asarray(low)


def complex_block(re, im):
    return np.block([[re, im], [-im, re]])


def make_tables(width, length, row_count, col_count):
    span = width // (row_count * col_count)
    n_count = span // SUB
    m_count = width // n_count
    rows = length // row_count
    m = np.arange(m_count)
    q = (np.arange(row_count)[:, None] * (col_count * SUB) + np.arange(SUB)[None, :]).reshape(-1)
    angle = 2 * np.pi * np.outer(m, q) / m_count
    forward_y = halves(complex_block(np.cos(angle), -np.sin(angle)))
    inverse_y = halves(complex_block(np.cos(angle.T), np.sin(angle.T)))
    i = np.arange(rows)
    angle = 2 * np.pi * np.outer(i, i) / rows
    forward_x = halves(complex_block(np.cos(angle), -np.sin(angle)))
    inverse_x = halves(complex_block(np.cos(angle), np.sin(angle)))
    k = np.arange(n_count)
    col = np.arange(col_count)[:, None, None]
    angle = 2 * np.pi * (k[:, None] * m[None, :] / width + col * SUB * m[None, None, :] / m_count)
    angle = angle + np.pi * col * k[:, None]
    norm = 1 / math.sqrt(width)
    turn_y = np.stack([np.cos(angle), np.sin(angle)], 2) * norm
    k = np.arange(row_count)
    angle = 2 * np.pi * np.outer(k, i) / length
    turn_x = np.stack([np.cos(angle), np.sin(angle)], 1) / math.sqrt(length)
    return dict(
        forward_y=forward_y,
        inverse_y=inverse_y,
        forward_x=forward_x,
        inverse_x=inverse_x,
        turn_y=jnp.asarray(turn_y, f32),
        turn_x=jnp.asarray(turn_x, f32),
    )


def split(z):
    high = z.astype(bf16)
    return high, (z - high.astype(f32)).astype(bf16)


def product(z, table_high, table_low):
    high, low = split(z)
    dot = functools.partial(jnp.dot, preferred_element_type=f32)
    return dot(high, table_high) + dot(low, table_high) + dot(high, table_low)


def group_of(count, rows):
    group = count
    while group > 1 and group * rows > 512:
        group //= 2
    return group


def lane_width(count):
    return min(LANES, count)


def forward_y_kernel(n_count, own, other, turn, table_high, table_low, out, work):
    rows = own.shape[0]
    m_count = turn.shape[2]
    lane = lane_width(m_count)
    half = n_count // 2

    def tile(t, carry):
        at = pl.ds(pl.multiple_of(t * SUB, SUB), SUB)
        for j in range(m_count // lane):
            xs = []
            for ref in (own, other):
                for n in range(half):
                    begin = n * m_count + j * lane
                    xs.append(ref[at, begin : begin + lane])
            spectrum = rfft_list(xs)
            for k in range(n_count):
                z = spectrum[k] if k <= half else conj(spectrum[n_count - k])
                c = turn[k, 0:1, j * lane : (j + 1) * lane]
                s = turn[k, 1:2, j * lane : (j + 1) * lane]
                if z[1] is None:
                    re, im = z[0] * c, z[0] * -s
                else:
                    re, im = z[0] * c + z[1] * s, z[1] * c - z[0] * s
                work[k, at, j * lane : (j + 1) * lane] = re
                work[k, at, m_count + j * lane : m_count + (j + 1) * lane] = im
        return carry

    lax.fori_loop(0, rows // SUB, tile, 0)
    group = group_of(n_count, rows)
    row_count = out.shape[0]
    q_count = row_count * SUB
    for g in range(0, n_count, group):
        z = work[g : g + group].reshape(group * rows, 2 * m_count)
        o = product(z, table_high[...], table_low[...])
        for k in range(group):
            for c in range(2):
                block = o[k * rows : (k + 1) * rows, c * q_count : (c + 1) * q_count]
                begin = (g + k) * SUB
                out[:, c, begin : begin + SUB, :] = block.T.reshape(row_count, SUB, rows)


def middle_kernel(
    last, data, turn, forward_high, forward_low, inverse_high, inverse_low, first_kernel, load, *rest
):
    if last:
        out, work = rest
    else:
        second_kernel, later_load, out, later_out, work = rest
    row_count, _, span, rows = data.shape

    def gather(t, carry):
        at = pl.ds(pl.multiple_of(t * SUB, SUB), SUB)
        zs = fft_list([(data[s, 0, at, :], data[s, 1, at, :]) for s in range(row_count)], -1.0)
        for k in range(row_count):
            c, s = turn[k, 0:1, :], turn[k, 1:2, :]
            work[k, at, :rows] = zs[k][0] * c + zs[k][1] * s
            work[k, at, rows:] = zs[k][1] * c - zs[k][0] * s
        return carry

    lax.fori_loop(0, span // SUB, gather, 0)
    group = group_of(row_count, span)
    for g in range(0, row_count, group):
        z = work[g : g + group].reshape(group * span, 2 * rows)
        spectrum = product(z, forward_high[...], forward_low[...]).reshape(group, span, 2 * rows)
        parts = (spectrum[:, :, :rows], spectrum[:, :, rows:])
        factor = first_kernel[g : g + group]
        loads = [load[c, g : g + group] + factor * parts[c] for c in range(2)]
        if not last:
            factor = second_kernel[g : g + group]
            for c in range(2):
                later_out[c, g : g + group] = later_load[c, g : g + group] + factor * parts[c]
        w = jnp.concatenate(loads, axis=2).reshape(group * span, 2 * rows)
        w = product(w, inverse_high[...], inverse_low[...])
        work[g : g + group] = w.reshape(group, span, 2 * rows)

    def scatter(t, carry):
        at = pl.ds(pl.multiple_of(t * SUB, SUB), SUB)
        zs = []
        for k in range(row_count):
            c, s = turn[k, 0:1, :], turn[k, 1:2, :]
            re, im = work[k, at, :rows], work[k, at, rows:]
            zs.append((re * c - im * s, im * c + re * s))
        zs = fft_list(zs, 1.0)
        for k in range(row_count):
            out[k, 0, at, :] = zs[k][0]
            out[k, 1, at, :] = zs[k][1]
        return carry

    lax.fori_loop(0, span // SUB, scatter, 0)


def inverse_y_kernel(n_count, data, turn, table_high, table_low, own, other, work):
    row_count, _, _, rows = data.shape
    m_count = turn.shape[2]
    lane = lane_width(m_count)
    half = n_count // 2
    q_count = row_count * SUB
    group = group_of(n_count, rows)
    for g in range(0, n_count, group):
        blocks = []
        for k in range(g, g + group):
            parts = [data[:, c, k * SUB : (k + 1) * SUB, :].reshape(q_count, rows).T for c in range(2)]
            blocks.append(jnp.concatenate(parts, axis=1))
        z = jnp.concatenate(blocks, axis=0)
        o = product(z, table_high[...], table_low[...])
        work[g : g + group] = o.reshape(group, rows, 2 * m_count)

    def tile(t, carry):
        at = pl.ds(pl.multiple_of(t * SUB, SUB), SUB)
        for j in range(m_count // lane):
            ys = []
            for k in range(n_count):
                c = turn[k, 0:1, j * lane : (j + 1) * lane]
                s = turn[k, 1:2, j * lane : (j + 1) * lane]
                re = work[k, at, j * lane : (j + 1) * lane]
                im = work[k, at, m_count + j * lane : m_count + (j + 1) * lane]
                ys.append((re * c - im * s, im * c + re * s))
            ps = [(ys[0][0], None)]
            for k in range(1, half):
                both = cadd(ys[k], conj(ys[n_count - k]))
                ps.append((both[0] * 0.5, both[1] * 0.5))
            ps.append((ys[half][0], None))
            xs = irfft_list(ps)
            for n in range(half):
                begin = n * m_count + j * lane
                own[at, begin : begin + lane] = xs[n]
                other[at, begin : begin + lane] = xs[half + n]
        return carry

    lax.fori_loop(0, rows // SUB, tile, 0)


def load_kernel(kernel, history, loads, later_loads, first, second, sums, turned):
    horizon, block, length = kernel.shape
    step = pl.program_id(0)
    lane = lane_width(length)
    at = pl.ds(pl.multiple_of(step * block, block), block)

    def chunk(j, carry):
        cols = pl.ds(pl.multiple_of(j * lane, lane), lane)
        totals = [jnp.zeros((block, lane), f32) for _ in range(4)]
        factors = [kernel[h, :, cols].astype(f32) for h in range(horizon)]
        for h in range(horizon - 1):
            for c in range(2):
                past = history[h, c, :, cols].astype(f32)
                totals[c] = totals[c] + factors[h + 1] * past
                if h + 2 < horizon:
                    totals[2 + c] = totals[2 + c] + factors[h + 2] * past
        for a, total in enumerate((*totals, factors[0], factors[1])):
            sums[a, j, at, :] = total
        return carry

    lax.fori_loop(0, length // lane, chunk, 0)

    @pl.when(step == pl.num_programs(0) - 1)
    def _():
        span = sums.shape[2]
        n_count = span // SUB
        row_count, _, rows = first.shape

        def reorder(a, target):
            for j in range(length // lane):
                pieces = [sums[a, j, pl.ds(k, SUB, stride=n_count), :] for k in range(n_count)]
                turned[j * lane : (j + 1) * lane, :span] = jnp.concatenate(pieces, axis=0).T
            for k in range(row_count):
                target[k] = turned[pl.ds(k, rows, stride=row_count), :][:, :span].T

        reorder(0, loads.at[0])
        reorder(1, loads.at[1])
        reorder(2, later_loads.at[0])
        reorder(3, later_loads.at[1])
        reorder(4, first)
        reorder(5, second)


def stencil_kernel(current, previous, slip, cells, above, below, beside, base, strength, following, grown):
    rows, cols = slip.shape
    lane = beside.shape[2] // 2
    row_index = lax.broadcasted_iota(jnp.int32, (rows, cols), 0)
    col_index = lax.broadcasted_iota(jnp.int32, (rows, cols), 1)
    for layer in range(2):
        here = current[layer]
        up = pltpu.roll(here, 1, 0)
        up = jnp.where(row_index == 0, above[layer, SUB - 1 : SUB, :], up)
        down = pltpu.roll(here, rows - 1, 0)
        down = jnp.where(row_index == rows - 1, below[layer, 0:1, :], down)
        left = pltpu.roll(here, 1, 1)
        left = jnp.where(col_index == 0, beside[layer, :, 2 * lane - 1 : 2 * lane], left)
        right = pltpu.roll(here, cols - 1, 1)
        right = jnp.where(col_index == cols - 1, beside[layer, :, 0:1], right)
        flat = up + down + left + right - 4.0 * here
        if layer == 0:
            across = current[1] + here - 2.0 * here
        else:
            across = current[0] - 2.0 * here
        following[layer] = 2.0 * here - previous[layer] + courant * (flat + across)
    count = cells.shape[1]
    for r in range(count):
        at = slice(r * BLOCK_CELLS, (r + 1) * BLOCK_CELLS)
        rate = current[0, at, :] - previous[0, at, :]
        old = slip[at, :]
        base[at, :] = cells[3, r : r + 1, :] - damping * rate
        weak = jnp.minimum(old * cells[2, r : r + 1, :], 1.0)
        strength[at, :] = cells[0, r : r + 1, :] - cells[1, r : r + 1, :] * weak
        grown[at, :] = old + jnp.abs(rate)


def traction_kernel(own, other, base, strength, current, partial, following, result):
    limit = strength[...]
    traction = jnp.clip(base[...] + (own[...] + other[...]), -limit, limit)
    updated = partial[0] + courant * traction
    following[0] = updated
    result[...] = updated - current[0]


def last_traction_kernel(own, other, base, strength, partial, following, result):
    limit = strength[...]
    traction = jnp.clip(base[...] + (own[...] + other[...]), -limit, limit)
    result[...] = traction
    following[0] = partial[0] + courant * traction


def vmem():
    return pl.BlockSpec(memory_space=pltpu.VMEM)


def call(kernel, inputs, outputs, scratch=(), flops=0, name=None):
    size = sum(int(np.prod(v.shape)) * v.dtype.itemsize for v in (*inputs, *outputs))
    return pl.pallas_call(
        kernel,
        in_specs=[vmem()] * len(inputs),
        out_specs=[vmem()] * len(outputs),
        out_shape=list(outputs),
        scratch_shapes=list(scratch),
        cost_estimate=pl.CostEstimate(flops=flops, transcendentals=0, bytes_accessed=size),
        name=name,
    )(*inputs)


def shards(
    wave_now,
    wave_before,
    fault_slip,
    region_ids,
    mode_history,
    wave_kernel,
    static_friction,
    dynamic_friction,
    weakening_slip,
    normal_stress,
    initial_stress,
):
    rows, cols = wave_now.shape[1], wave_now.shape[2]
    row_count = lax.axis_size("row")
    col_count = lax.axis_size("col")
    assert col_count == 2 and SUBSTEPS == 2
    width, length = cols * col_count, rows * row_count
    span = width // (row_count * col_count)
    n_count = span // SUB
    m_count = width // n_count
    horizon = mode_history.shape[0]
    tables = make_tables(width, length, row_count, col_count)
    turn_y = lax.dynamic_index_in_dim(tables["turn_y"], lax.axis_index("col"), 0, keepdims=False)
    half_shape = jax.ShapeDtypeStruct((row_count, 2, span, rows), f32)
    tile_shape = jax.ShapeDtypeStruct((rows, cols), f32)
    load_shape = jax.ShapeDtypeStruct((2, row_count, span, rows), f32)
    factor_shape = jax.ShapeDtypeStruct((row_count, span, rows), f32)

    def swap(value):
        return lax.ppermute(value, "col", [(0, 1), (1, 0)])

    def regroup(value):
        return lax.all_to_all(value, "row", split_axis=0, concat_axis=0, tiled=True)

    chosen = region_ids[None] == jnp.arange(static_friction.shape[0], dtype=jnp.int32)[:, None, None]

    def lookup(table):
        return jnp.sum(jnp.where(chosen, table[:, None, None], 0.0), axis=0)

    normal_load = lookup(normal_stress)
    static_level = lookup(static_friction)
    blocks = jnp.stack(
        [
            normal_load * static_level,
            normal_load * (static_level - lookup(dynamic_friction)),
            1.0 / lookup(weakening_slip),
            lookup(initial_stress),
        ]
    )
    spread = np.repeat(np.eye(region_ids.shape[1], dtype=np.float32), BLOCK_CELLS, axis=1)
    cells = jnp.einsum("abc,cd->abd", blocks, spread, precision=lax.Precision.HIGHEST)

    block = 16
    past = jax.ShapeDtypeStruct
    loads, later_loads, first, second = pl.pallas_call(
        load_kernel,
        grid=(span // block,),
        in_specs=[
            pl.BlockSpec((horizon, block, length), lambda b: (0, b, 0)),
            pl.BlockSpec((horizon - 1, 2, block, length), lambda b: (0, 0, b, 0)),
        ],
        out_specs=[vmem()] * 4,
        out_shape=[load_shape, load_shape, factor_shape, factor_shape],
        scratch_shapes=[
            pltpu.VMEM((6, length // lane_width(length), span, lane_width(length)), f32),
            pltpu.VMEM((length, max(span, LANES)), f32),
        ],
        cost_estimate=pl.CostEstimate(
            flops=20 * horizon * span * length, transcendentals=0, bytes_accessed=6 * horizon * span * length
        ),
        name="past_loads",
    )(wave_kernel, mode_history)

    def forward(rate):
        work = pltpu.VMEM((n_count, rows, 2 * m_count), f32)
        inputs = (rate, swap(rate), turn_y, *tables["forward_y"])
        (part,) = call(
            functools.partial(forward_y_kernel, n_count), inputs, [half_shape], [work], 10**9, "forward_y"
        )
        return regroup(part)

    def middle(last, data, *more):
        work = pltpu.VMEM((row_count, span, 2 * rows), f32)
        outputs = [half_shape] if last else [half_shape, load_shape]
        inputs = (data, tables["turn_x"], *tables["forward_x"], *tables["inverse_x"], *more)
        return call(functools.partial(middle_kernel, last), inputs, outputs, [work], 10**9, "middle")

    def inverse(data):
        work = pltpu.VMEM((n_count, rows, 2 * m_count), f32)
        own, other = call(
            functools.partial(inverse_y_kernel, n_count),
            (data, turn_y, *tables["inverse_y"]),
            [tile_shape, tile_shape],
            [work],
            10**9,
            "inverse_y",
        )
        return own, swap(other)

    def stencil(current, previous, slip):
        ring = [(i, (i + 1) % row_count) for i in range(row_count)]
        above = lax.ppermute(current[:, rows - SUB :], "row", ring)
        below = lax.ppermute(current[:, :SUB], "row", [(b, a) for a, b in ring])
        edge = lane_width(cols)
        beside = swap(jnp.concatenate([current[:, :, :edge], current[:, :, cols - edge :]], axis=2))
        inputs = (current, previous, slip, cells, above, below, beside)
        outputs = [tile_shape, tile_shape, jax.ShapeDtypeStruct(current.shape, f32), tile_shape]
        return call(stencil_kernel, inputs, outputs, (), 5 * 10**8, "stencil")

    def traction_step(kernel, *inputs):
        step = 32 if rows % 32 == 0 else rows
        layer = pl.BlockSpec((1, step, cols), lambda i: (0, i, 0))
        tile = pl.BlockSpec((step, cols), lambda i: (i, 0))
        partial = inputs[-1]
        specs = [layer if v.ndim == 3 else tile for v in inputs]
        return pl.pallas_call(
            kernel,
            grid=(rows // step,),
            in_specs=specs,
            out_specs=[layer, tile],
            out_shape=[jax.ShapeDtypeStruct(partial.shape, f32), tile_shape],
            input_output_aliases={len(inputs) - 1: 0},
            name="traction",
        )(*inputs)

    data = forward(wave_now[0] - wave_before[0])
    base, strength, partial, slip = stencil(wave_now, wave_before, fault_slip)
    back, later_loads = middle(False, data, first, loads, second, later_loads)
    own, other = inverse(regroup(back))
    current, rate = traction_step(traction_kernel, own, other, base, strength, wave_now, partial)

    data = forward(rate)
    base, strength, partial, slip = stencil(current, wave_now, slip)
    (back,) = middle(True, data, first, later_loads)
    own, other = inverse(regroup(back))
    current, traction = traction_step(last_traction_kernel, own, other, base, strength, partial)
    return (current, slip, traction)


def solution(mesh):
    return jax.shard_map(
        shards,
        mesh=mesh,
        in_specs=(
            P("groups", "row", "col"),
            P("groups", "row", "col"),
            P(("groups", "row"), "col"),
            P(("groups", "row"), "col"),
            P("groups", None, ("row", "col"), None),
            P(None, ("row", "col"), None),
            P(),
            P(),
            P(),
            P(),
            P(),
        ),
        out_specs=(
            P("groups", "row", "col"),
            P(("groups", "row"), "col"),
            P(("groups", "row"), "col"),
        ),
        check_vma=False,
    )
```

```python
import functools
import math

import jax
import jax.numpy as jnp
import numpy as np
from jax import lax
from jax.experimental import pallas as pl
from jax.experimental.pallas import tpu as pltpu
from jax.sharding import PartitionSpec as P

SUBSTEPS = 2
BLOCK_CELLS = 16
LANES = 128
SUB = 8

damping = 0.5
courant = 0.3
f32 = jnp.float32
bf16 = jnp.bfloat16


def add(a, b):
    if a is None:
        return b
    return a if b is None else a + b


def sub(a, b):
    if b is None:
        return a
    return -b if a is None else a - b


def scale(z, w):
    re, im = z
    c, s = w.real, w.imag
    if abs(s) < 1e-12:
        return (re, im) if c > 0 else (-re, None if im is None else -im)
    if abs(c) < 1e-12:
        if s > 0:
            return (None if im is None else -im, re)
        return (im, None if re is None else -re)
    if im is None:
        return (re * c, re * s)
    if re is None:
        return (im * -s, im * c)
    if abs(abs(c) - abs(s)) < 1e-12:
        a = abs(c)
        signs = (c > 0, s > 0)
        if signs == (True, True):
            return ((re - im) * a, (re + im) * a)
        if signs == (True, False):
            return ((re + im) * a, (im - re) * a)
        if signs == (False, True):
            return ((re + im) * -a, (re - im) * a)
        return ((im - re) * a, (re + im) * -a)
    return (re * c - im * s, re * s + im * c)


def cadd(a, b):
    return (add(a[0], b[0]), add(a[1], b[1]))


def csub(a, b):
    return (sub(a[0], b[0]), sub(a[1], b[1]))


def conj(a):
    return (a[0], None if a[1] is None else -a[1])


def root(k, n, sign):
    return complex(math.cos(2 * math.pi * k / n), sign * math.sin(2 * math.pi * k / n))


def fft_list(zs, sign):
    n = len(zs)
    if n == 1:
        return list(zs)
    even = fft_list(zs[0::2], sign)
    odd = fft_list(zs[1::2], sign)
    low, high = [], []
    for k in range(n // 2):
        t = scale(odd[k], root(k, n, sign))
        low.append(cadd(even[k], t))
        high.append(csub(even[k], t))
    return low + high


def rfft_list(xs):
    n = len(xs)
    if n == 1:
        return [(xs[0], None)]
    if n == 2:
        return [(xs[0] + xs[1], None), (xs[0] - xs[1], None)]
    even = rfft_list(xs[0::2])
    odd = rfft_list(xs[1::2])
    out = [None] * (n // 2 + 1)
    for k in range(n // 4 + 1):
        t = scale(odd[k], root(k, n, -1.0))
        out[k] = cadd(even[k], t)
        if n // 2 - k != k:
            out[n // 2 - k] = conj(csub(even[k], t))
    return out


def irfft_list(ps):
    n = 2 * (len(ps) - 1)
    if n == 2:
        return [ps[0][0] + ps[1][0], ps[0][0] - ps[1][0]]
    even, odd = [], []
    for k in range(n // 4 + 1):
        mirrored = conj(ps[n // 2 - k])
        even.append(cadd(ps[k], mirrored))
        odd.append(scale(csub(ps[k], mirrored), root(k, n, 1.0)))
    a, b = irfft_list(even), irfft_list(odd)
    return [v for pair in zip(a, b) for v in pair]


def halves(table):
    high = table.astype(np.float32).astype(bf16)
    low = (table - high.astype(np.float64)).astype(np.float32).astype(bf16)
    return jnp.asarray(high), jnp.asarray(low)


def complex_block(re, im):
    return np.block([[re, im], [-im, re]])


def make_tables(width, length, row_count, col_count):
    span = width // (row_count * col_count)
    n_count = span // SUB
    m_count = width // n_count
    rows = length // row_count
    m = np.arange(m_count)
    q = (np.arange(row_count)[:, None] * (col_count * SUB) + np.arange(SUB)[None, :]).reshape(-1)
    angle = 2 * np.pi * np.outer(m, q) / m_count
    forward_y = halves(complex_block(np.cos(angle), -np.sin(angle)))
    i = np.arange(rows)
    angle = 2 * np.pi * np.outer(i, i) / rows
    forward_x = halves(complex_block(np.cos(angle), -np.sin(angle)))
    k = np.arange(n_count)
    col = np.arange(col_count)[:, None, None]
    angle = 2 * np.pi * (k[:, None] * m[None, :] / width + col * SUB * m[None, None, :] / m_count)
    angle = angle + np.pi * col * k[:, None]
    norm = 1 / math.sqrt(width)
    turn_y = np.stack([np.cos(angle), np.sin(angle)], 2) * norm
    k = np.arange(row_count)
    angle = 2 * np.pi * np.outer(k, i) / length
    turn_x = np.stack([np.cos(angle), np.sin(angle)], 1) / math.sqrt(length)
    return dict(
        table_y=forward_y,
        table_x=forward_x,
        turn_y=jnp.asarray(turn_y, f32),
        turn_x=jnp.asarray(turn_x, f32),
    )


def split(z):
    high = z.astype(bf16)
    return high, (z - high.astype(f32)).astype(bf16)


def product(z, table_high, table_low, inverse=False):
    high, low = split(z)

    def dot(a, b):
        return lax.dot_general(a, b, (((1,), (1 if inverse else 0,)), ((), ())), preferred_element_type=f32)

    return dot(high, table_high) + dot(low, table_high) + dot(high, table_low)


def group_of(count, rows):
    group = count
    while group > 1 and group * rows > 512:
        group //= 2
    return group


def lane_width(count):
    return min(LANES, count)


def forward_y_kernel(n_count, own, other, turn, table_high, table_low, out, work):
    rows = own.shape[0]
    m_count = turn.shape[2]
    lane = lane_width(m_count)
    half = n_count // 2

    def tile(t, carry):
        at = pl.ds(pl.multiple_of(t * SUB, SUB), SUB)
        for j in range(m_count // lane):
            xs = []
            for ref in (own, other):
                for n in range(half):
                    begin = n * m_count + j * lane
                    xs.append(ref[at, begin : begin + lane])
            spectrum = rfft_list(xs)
            for k in range(n_count):
                z = spectrum[k] if k <= half else conj(spectrum[n_count - k])
                c = turn[k, 0:1, j * lane : (j + 1) * lane]
                s = turn[k, 1:2, j * lane : (j + 1) * lane]
                if z[1] is None:
                    re, im = z[0] * c, z[0] * -s
                else:
                    re, im = z[0] * c + z[1] * s, z[1] * c - z[0] * s
                work[k, at, j * lane : (j + 1) * lane] = re
                work[k, at, m_count + j * lane : m_count + (j + 1) * lane] = im
        return carry

    lax.fori_loop(0, rows // SUB, tile, 0)
    group = group_of(n_count, rows)
    row_count = out.shape[0]
    q_count = row_count * SUB
    for g in range(0, n_count, group):
        z = work[g : g + group].reshape(group * rows, 2 * m_count)
        o = product(z, table_high[...], table_low[...])
        for k in range(group):
            for c in range(2):
                block = o[k * rows : (k + 1) * rows, c * q_count : (c + 1) * q_count]
                begin = (g + k) * SUB
                out[:, c, begin : begin + SUB, :] = block.T.reshape(row_count, SUB, rows)


def middle_kernel(
    last, data, turn, table_high, table_low, first_kernel, load, *rest
):
    if last:
        out, work = rest
    else:
        second_kernel, later_load, out, later_out, work = rest
    row_count, _, span, rows = data.shape

    def gather(t, carry):
        at = pl.ds(pl.multiple_of(t * SUB, SUB), SUB)
        zs = fft_list([(data[s, 0, at, :], data[s, 1, at, :]) for s in range(row_count)], -1.0)
        for k in range(row_count):
            c, s = turn[k, 0:1, :], turn[k, 1:2, :]
            work[k, at, :rows] = zs[k][0] * c + zs[k][1] * s
            work[k, at, rows:] = zs[k][1] * c - zs[k][0] * s
        return carry

    lax.fori_loop(0, span // SUB, gather, 0)
    group = group_of(row_count, span)
    for g in range(0, row_count, group):
        z = work[g : g + group].reshape(group * span, 2 * rows)
        spectrum = product(z, table_high[...], table_low[...]).reshape(group, span, 2 * rows)
        parts = (spectrum[:, :, :rows], spectrum[:, :, rows:])
        factor = first_kernel[g : g + group]
        loads = [load[c, g : g + group] + factor * parts[c] for c in range(2)]
        if not last:
            factor = second_kernel[g : g + group]
            for c in range(2):
                later_out[c, g : g + group] = later_load[c, g : g + group] + factor * parts[c]
        w = jnp.concatenate(loads, axis=2).reshape(group * span, 2 * rows)
        w = product(w, table_high[...], table_low[...], True)
        work[g : g + group] = w.reshape(group, span, 2 * rows)

    def scatter(t, carry):
        at = pl.ds(pl.multiple_of(t * SUB, SUB), SUB)
        zs = []
        for k in range(row_count):
            c, s = turn[k, 0:1, :], turn[k, 1:2, :]
            re, im = work[k, at, :rows], work[k, at, rows:]
            zs.append((re * c - im * s, im * c + re * s))
        zs = fft_list(zs, 1.0)
        for k in range(row_count):
            out[k, 0, at, :] = zs[k][0]
            out[k, 1, at, :] = zs[k][1]
        return carry

    lax.fori_loop(0, span // SUB, scatter, 0)


def inverse_y_kernel(n_count, data, turn, table_high, table_low, own, other, work):
    row_count, _, _, rows = data.shape
    m_count = turn.shape[2]
    lane = lane_width(m_count)
    half = n_count // 2
    q_count = row_count * SUB
    group = group_of(n_count, rows)
    for g in range(0, n_count, group):
        blocks = []
        for k in range(g, g + group):
            parts = [data[:, c, k * SUB : (k + 1) * SUB, :].reshape(q_count, rows).T for c in range(2)]
            blocks.append(jnp.concatenate(parts, axis=1))
        z = jnp.concatenate(blocks, axis=0)
        o = product(z, table_high[...], table_low[...], True)
        work[g : g + group] = o.reshape(group, rows, 2 * m_count)

    def tile(t, carry):
        at = pl.ds(pl.multiple_of(t * SUB, SUB), SUB)
        for j in range(m_count // lane):
            ys = []
            for k in range(n_count):
                c = turn[k, 0:1, j * lane : (j + 1) * lane]
                s = turn[k, 1:2, j * lane : (j + 1) * lane]
                re = work[k, at, j * lane : (j + 1) * lane]
                im = work[k, at, m_count + j * lane : m_count + (j + 1) * lane]
                ys.append((re * c - im * s, im * c + re * s))
            ps = [(ys[0][0], None)]
            for k in range(1, half):
                both = cadd(ys[k], conj(ys[n_count - k]))
                ps.append((both[0] * 0.5, both[1] * 0.5))
            ps.append((ys[half][0], None))
            xs = irfft_list(ps)
            for n in range(half):
                begin = n * m_count + j * lane
                own[at, begin : begin + lane] = xs[n]
                other[at, begin : begin + lane] = xs[half + n]
        return carry

    lax.fori_loop(0, rows // SUB, tile, 0)


def load_kernel(kernel, history, loads, later_loads, first, second, sums, turned):
    horizon, block, length = kernel.shape
    step = pl.program_id(0)
    lane = lane_width(length)
    at = pl.ds(pl.multiple_of(step * block, block), block)

    def chunk(j, carry):
        cols = pl.ds(pl.multiple_of(j * lane, lane), lane)
        totals = [jnp.zeros((block, lane), f32) for _ in range(4)]
        factors = [kernel[h, :, cols].astype(f32) for h in range(horizon)]
        for h in range(horizon - 1):
            for c in range(2):
                past = history[h, c, :, cols].astype(f32)
                totals[c] = totals[c] + factors[h + 1] * past
                if h + 2 < horizon:
                    totals[2 + c] = totals[2 + c] + factors[h + 2] * past
        for a, total in enumerate((*totals, factors[0], factors[1])):
            sums[a, j, at, :] = total
        return carry

    lax.fori_loop(0, length // lane, chunk, 0)

    @pl.when(step == pl.num_programs(0) - 1)
    def _():
        span = sums.shape[2]
        n_count = span // SUB
        row_count, _, rows = first.shape

        def reorder(a, target):
            for j in range(length // lane):
                pieces = [sums[a, j, pl.ds(k, SUB, stride=n_count), :] for k in range(n_count)]
                turned[j * lane : (j + 1) * lane, :span] = jnp.concatenate(pieces, axis=0).T
            for k in range(row_count):
                target[k] = turned[pl.ds(k, rows, stride=row_count), :][:, :span].T

        reorder(0, loads.at[0])
        reorder(1, loads.at[1])
        reorder(2, later_loads.at[0])
        reorder(3, later_loads.at[1])
        reorder(4, first)
        reorder(5, second)


def stencil_kernel(
    lower, upper, old_lower, old_upper, slip, cells, above, below, beside, base, strength, partial, following, grown
):
    rows, cols = slip.shape
    lane = beside.shape[2] // 2
    row_index = lax.broadcasted_iota(jnp.int32, (rows, cols), 0)
    col_index = lax.broadcasted_iota(jnp.int32, (rows, cols), 1)
    layers = ((lower, old_lower, upper, partial), (upper, old_upper, lower, following))
    for layer, (now, before, across, target) in enumerate(layers):
        here = now[0]
        up = pltpu.roll(here, 1, 0)
        up = jnp.where(row_index == 0, above[layer, SUB - 1 : SUB, :], up)
        down = pltpu.roll(here, rows - 1, 0)
        down = jnp.where(row_index == rows - 1, below[layer, 0:1, :], down)
        left = pltpu.roll(here, 1, 1)
        left = jnp.where(col_index == 0, beside[layer, :, 2 * lane - 1 : 2 * lane], left)
        right = pltpu.roll(here, cols - 1, 1)
        right = jnp.where(col_index == cols - 1, beside[layer, :, 0:1], right)
        flat = up + down + left + right - 4.0 * here
        normal = across[0] - 2.0 * here if layer else across[0] + here - 2.0 * here
        target[0] = 2.0 * here - before[0] + courant * (flat + normal)
    for r in range(cells.shape[1]):
        at = slice(r * BLOCK_CELLS, (r + 1) * BLOCK_CELLS)
        rate = lower[0, at, :] - old_lower[0, at, :]
        old = slip[at, :]
        base[at, :] = cells[3, r : r + 1, :] - damping * rate
        weak = jnp.minimum(old * cells[2, r : r + 1, :], 1.0)
        strength[at, :] = cells[0, r : r + 1, :] - cells[1, r : r + 1, :] * weak
        grown[at, :] = old + jnp.abs(rate)


def clipped(own, other, base, strength):
    limit = strength[...]
    return jnp.clip(base[...] + (own[...] + other[...]), -limit, limit)


def traction_kernel(own, other, base, strength, partial, current, following, rate):
    updated = partial[0] + courant * clipped(own, other, base, strength)
    following[0] = updated
    rate[...] = updated - current[0]


def last_traction_kernel(own, other, base, strength, partial, whole, following, result):
    traction = clipped(own, other, base, strength)
    result[...] = traction
    following[0] = partial[0] + courant * traction


def vmem():
    return pl.BlockSpec(memory_space=pltpu.VMEM)


def call(kernel, inputs, outputs, scratch=(), flops=0, name=None, limit=20 * 2**20):
    size = sum(int(np.prod(v.shape)) * v.dtype.itemsize for v in (*inputs, *outputs))
    return pl.pallas_call(
        kernel,
        in_specs=[vmem()] * len(inputs),
        out_specs=[vmem()] * len(outputs),
        out_shape=list(outputs),
        scratch_shapes=list(scratch),
        cost_estimate=pl.CostEstimate(flops=flops, transcendentals=0, bytes_accessed=size),
        name=name,
        compiler_params=pltpu.CompilerParams(vmem_limit_bytes=limit),
    )(*inputs)


def shards(
    wave_now,
    wave_before,
    fault_slip,
    region_ids,
    mode_history,
    wave_kernel,
    static_friction,
    dynamic_friction,
    weakening_slip,
    normal_stress,
    initial_stress,
):
    rows, cols = wave_now.shape[1], wave_now.shape[2]
    row_count = lax.axis_size("row")
    col_count = lax.axis_size("col")
    assert col_count == 2 and SUBSTEPS == 2
    width, length = cols * col_count, rows * row_count
    span = width // (row_count * col_count)
    n_count = span // SUB
    m_count = width // n_count
    horizon = mode_history.shape[0]
    tables = make_tables(width, length, row_count, col_count)
    turn_y = lax.dynamic_index_in_dim(tables["turn_y"], lax.axis_index("col"), 0, keepdims=False)
    half_shape = jax.ShapeDtypeStruct((row_count, 2, span, rows), f32)
    tile_shape = jax.ShapeDtypeStruct((rows, cols), f32)
    load_shape = jax.ShapeDtypeStruct((2, row_count, span, rows), f32)
    factor_shape = jax.ShapeDtypeStruct((row_count, span, rows), f32)

    def swap(value):
        return lax.ppermute(value, "col", [(0, 1), (1, 0)])

    def regroup(value):
        return lax.all_to_all(value, "row", split_axis=0, concat_axis=0, tiled=True)

    chosen = region_ids[None] == jnp.arange(static_friction.shape[0], dtype=jnp.int32)[:, None, None]

    def lookup(table):
        return jnp.sum(jnp.where(chosen, table[:, None, None], 0.0), axis=0)

    normal_load = lookup(normal_stress)
    static_level = lookup(static_friction)
    blocks = jnp.stack(
        [
            normal_load * static_level,
            normal_load * (static_level - lookup(dynamic_friction)),
            1.0 / lookup(weakening_slip),
            lookup(initial_stress),
        ]
    )
    block_of = lax.broadcasted_iota(jnp.int32, (region_ids.shape[1], cols), 1) // BLOCK_CELLS
    spread = (block_of == lax.broadcasted_iota(jnp.int32, block_of.shape, 0)).astype(f32)
    cells = jnp.einsum("abc,cd->abd", blocks, spread, precision=lax.Precision.HIGHEST)

    block = 16
    past = jax.ShapeDtypeStruct
    loads, later_loads, first, second = pl.pallas_call(
        load_kernel,
        grid=(span // block,),
        in_specs=[
            pl.BlockSpec((horizon, block, length), lambda b: (0, b, 0)),
            pl.BlockSpec((horizon - 1, 2, block, length), lambda b: (0, 0, b, 0)),
        ],
        out_specs=[vmem()] * 4,
        out_shape=[load_shape, load_shape, factor_shape, factor_shape],
        scratch_shapes=[
            pltpu.VMEM((6, length // lane_width(length), span, lane_width(length)), f32),
            pltpu.VMEM((length, max(span, LANES)), f32),
        ],
        cost_estimate=pl.CostEstimate(
            flops=20 * horizon * span * length, transcendentals=0, bytes_accessed=6 * horizon * span * length
        ),
        name="past_loads",
        compiler_params=pltpu.CompilerParams(vmem_limit_bytes=32 * 2**20),
    )(wave_kernel, mode_history)

    def forward(rate):
        work = pltpu.VMEM((n_count, rows, 2 * m_count), f32)
        inputs = (rate, swap(rate), turn_y, *tables["table_y"])
        (part,) = call(
            functools.partial(forward_y_kernel, n_count), inputs, [half_shape], [work], 10**9, "forward_y"
        )
        return regroup(part)

    def middle(last, data, *more):
        work = pltpu.VMEM((row_count, span, 2 * rows), f32)
        outputs = [half_shape] if last else [half_shape, load_shape]
        inputs = (data, tables["turn_x"], *tables["table_x"], *more)
        return call(functools.partial(middle_kernel, last), inputs, outputs, [work], 10**9, "middle")

    def inverse(data):
        work = pltpu.VMEM((n_count, rows, 2 * m_count), f32)
        own, other = call(
            functools.partial(inverse_y_kernel, n_count),
            (data, turn_y, *tables["table_y"]),
            [tile_shape, tile_shape],
            [work],
            10**9,
            "inverse_y",
        )
        return own, swap(other)

    ring = [(i, (i + 1) % row_count) for i in range(row_count)]
    edge = lane_width(cols)
    layer_shape = jax.ShapeDtypeStruct((1, rows, cols), f32)

    def stencil(last, lower, upper, old_lower, old_upper, slip):
        def edges(begin, size, axis):
            pick = lambda v: lax.slice_in_dim(v[0][v[1] : v[1] + 1], begin, begin + size, axis=axis)
            return jnp.concatenate([pick(lower), pick(upper)], axis=0)

        above = lax.ppermute(edges(rows - SUB, SUB, 1), "row", ring)
        below = lax.ppermute(edges(0, SUB, 1), "row", [(b, a) for a, b in ring])
        beside = swap(jnp.concatenate([edges(0, edge, 2), edges(cols - edge, edge, 2)], axis=2))
        layers = (lower, upper, old_lower, old_upper)
        more = (slip, cells, above, below, beside)

        def at_layer(index):
            return pl.BlockSpec((1, rows, cols), lambda i: (index, 0, 0))

        following = jax.ShapeDtypeStruct((2, rows, cols), f32) if last else layer_shape
        specs = [tile_shape, tile_shape, layer_shape, following, tile_shape]
        whole = pl.BlockSpec((rows, cols), lambda i: (0, 0))
        return pl.pallas_call(
            stencil_kernel,
            grid=(1,),
            in_specs=[at_layer(index) for _, index in layers] + [vmem()] * len(more),
            out_specs=[whole, whole, at_layer(0), at_layer(1 if last else 0), whole],
            out_shape=specs,
            cost_estimate=pl.CostEstimate(flops=5 * 10**9, transcendentals=0, bytes_accessed=40 * rows * cols),
            compiler_params=pltpu.CompilerParams(vmem_limit_bytes=40 * 2**20),
            name="stencil",
        )(*[v for v, _ in layers], *more)

    def traction_step(last, own, other, base, strength, partial, extra):
        step = 32 if rows % 32 == 0 else rows
        layer = pl.BlockSpec((1, step, cols), lambda i: (0, i, 0))
        tile = pl.BlockSpec((step, cols), lambda i: (i, 0))
        return pl.pallas_call(
            last_traction_kernel if last else traction_kernel,
            grid=(rows // step,),
            in_specs=[tile] * 4 + [layer, pl.BlockSpec(memory_space=pl.ANY) if last else layer],
            out_specs=[layer, tile],
            out_shape=[jax.ShapeDtypeStruct(extra.shape if last else (1, rows, cols), f32), tile_shape],
            input_output_aliases={5: 0} if last else {},
            compiler_params=pltpu.CompilerParams(vmem_limit_bytes=12 * 2**20),
            name="traction",
        )(own, other, base, strength, partial, extra)

    data = forward(wave_now[0] - wave_before[0])
    found = stencil(False, (wave_now, 0), (wave_now, 1), (wave_before, 0), (wave_before, 1), fault_slip)
    data, (loads, later_loads, first, second), found = lax.optimization_barrier(
        (data, (loads, later_loads, first, second), found)
    )
    base, strength, partial, upper, slip = found
    back, later_loads = middle(False, data, first, loads, second, later_loads)
    own, other = inverse(regroup(back))
    lower, rate = traction_step(False, own, other, base, strength, partial, wave_now)

    data = forward(rate)
    found = stencil(True, (lower, 0), (upper, 0), (wave_now, 0), (wave_now, 1), slip)
    data, found = lax.optimization_barrier((data, found))
    base, strength, partial, following, slip = found
    (back,) = middle(True, data, first, later_loads)
    own, other = inverse(regroup(back))
    current, traction = traction_step(True, own, other, base, strength, partial, following)
    return (current, slip, traction)


def solution(mesh):
    return jax.shard_map(
        shards,
        mesh=mesh,
        in_specs=(
            P("groups", "row", "col"),
            P("groups", "row", "col"),
            P(("groups", "row"), "col"),
            P(("groups", "row"), "col"),
            P("groups", None, ("row", "col"), None),
            P(None, ("row", "col"), None),
            P(),
            P(),
            P(),
            P(),
            P(),
        ),
        out_specs=(
            P("groups", "row", "col"),
            P(("groups", "row"), "col"),
            P(("groups", "row"), "col"),
        ),
        check_vma=False,
    )
```

```python
import functools
import math

import jax
import jax.numpy as jnp
import numpy as np
from jax import lax
from jax.experimental import pallas as pl
from jax.experimental.pallas import tpu as pltpu
from jax.sharding import PartitionSpec as P

SUBSTEPS = 2
BLOCK_CELLS = 16
LANES = 128
MAX_PERMUTES = 16
SUB = 8

damping = 0.5
courant = 0.3
f32 = jnp.float32
bf16 = jnp.bfloat16


def add(a, b):
    if a is None:
        return b
    return a if b is None else a + b


def sub(a, b):
    if b is None:
        return a
    return -b if a is None else a - b


def scale(z, w):
    re, im = z
    c, s = w.real, w.imag
    if abs(s) < 1e-12:
        return (re, im) if c > 0 else (-re, None if im is None else -im)
    if abs(c) < 1e-12:
        if s > 0:
            return (None if im is None else -im, re)
        return (im, None if re is None else -re)
    if im is None:
        return (re * c, re * s)
    if re is None:
        return (im * -s, im * c)
    if abs(abs(c) - abs(s)) < 1e-12:
        a = abs(c)
        signs = (c > 0, s > 0)
        if signs == (True, True):
            return ((re - im) * a, (re + im) * a)
        if signs == (True, False):
            return ((re + im) * a, (im - re) * a)
        if signs == (False, True):
            return ((re + im) * -a, (re - im) * a)
        return ((im - re) * a, (re + im) * -a)
    return (re * c - im * s, re * s + im * c)


def cadd(a, b):
    return (add(a[0], b[0]), add(a[1], b[1]))


def csub(a, b):
    return (sub(a[0], b[0]), sub(a[1], b[1]))


def conj(a):
    return (a[0], None if a[1] is None else -a[1])


def root(k, n, sign):
    return complex(math.cos(2 * math.pi * k / n), sign * math.sin(2 * math.pi * k / n))


def fft_list(zs, sign):
    n = len(zs)
    if n == 1:
        return list(zs)
    even = fft_list(zs[0::2], sign)
    odd = fft_list(zs[1::2], sign)
    low, high = [], []
    for k in range(n // 2):
        t = scale(odd[k], root(k, n, sign))
        low.append(cadd(even[k], t))
        high.append(csub(even[k], t))
    return low + high


def rfft_list(xs):
    n = len(xs)
    if n == 1:
        return [(xs[0], None)]
    if n == 2:
        return [(xs[0] + xs[1], None), (xs[0] - xs[1], None)]
    even = rfft_list(xs[0::2])
    odd = rfft_list(xs[1::2])
    out = [None] * (n // 2 + 1)
    for k in range(n // 4 + 1):
        t = scale(odd[k], root(k, n, -1.0))
        out[k] = cadd(even[k], t)
        if n // 2 - k != k:
            out[n // 2 - k] = conj(csub(even[k], t))
    return out


def irfft_list(ps):
    n = 2 * (len(ps) - 1)
    if n == 2:
        return [ps[0][0] + ps[1][0], ps[0][0] - ps[1][0]]
    even, odd = [], []
    for k in range(n // 4 + 1):
        mirrored = conj(ps[n // 2 - k])
        even.append(cadd(ps[k], mirrored))
        odd.append(scale(csub(ps[k], mirrored), root(k, n, 1.0)))
    a, b = irfft_list(even), irfft_list(odd)
    return [v for pair in zip(a, b) for v in pair]


def halves(table):
    high = table.astype(np.float32).astype(bf16)
    low = (table - high.astype(np.float64)).astype(np.float32).astype(bf16)
    return jnp.asarray(high), jnp.asarray(low)


def complex_block(re, im):
    return np.block([[re, im], [-im, re]])


def table_of(count, picked):
    angle = 2 * np.pi * np.outer(np.arange(count), picked) / count
    return halves(complex_block(np.cos(angle), -np.sin(angle)))


def phases(index, period, norm):
    angle = (index % period).astype(f32) * (2 * math.pi / period)
    return jnp.stack([jnp.cos(angle), jnp.sin(angle)], axis=1) * norm


def split(z):
    high = z.astype(bf16)
    return high, (z - high.astype(f32)).astype(bf16)


def product(z, table_high, table_low, inverse=False):
    high, low = split(z)

    def dot(a, b):
        return lax.dot_general(a, b, (((1,), (1 if inverse else 0,)), ((), ())), preferred_element_type=f32)

    return dot(high, table_high) + dot(low, table_high) + dot(high, table_low)


def group_of(count, rows):
    group = count
    while group > 1 and group * rows > 512:
        group //= 2
    return group


def in_order(order, refs):
    placed = [None] * len(order)
    for place, ref in zip(order, refs):
        placed[place] = ref
    return placed


def lane_width(count):
    return min(LANES, count)


def forward_y_kernel(n_count, own, other, turn, table_high, table_low, *rest):
    *out, work = rest
    rows = own.shape[0]
    m_count = turn.shape[2]
    lane = lane_width(m_count)
    half = n_count // 2

    def tile(t, carry):
        at = pl.ds(pl.multiple_of(t * SUB, SUB), SUB)
        for j in range(m_count // lane):
            xs = []
            for ref in (own, other):
                for n in range(half):
                    begin = n * m_count + j * lane
                    xs.append(ref[at, begin : begin + lane])
            spectrum = rfft_list(xs)
            for k in range(n_count):
                z = spectrum[k] if k <= half else conj(spectrum[n_count - k])
                c = turn[k, 0:1, j * lane : (j + 1) * lane]
                s = turn[k, 1:2, j * lane : (j + 1) * lane]
                if z[1] is None:
                    re, im = z[0] * c, z[0] * -s
                else:
                    re, im = z[0] * c + z[1] * s, z[1] * c - z[0] * s
                work[k, at, j * lane : (j + 1) * lane] = re
                work[k, at, m_count + j * lane : m_count + (j + 1) * lane] = im
        return carry

    lax.fori_loop(0, rows // SUB, tile, 0)
    group = group_of(n_count, rows)
    q_count = len(out) * SUB
    for g in range(0, n_count, group):
        z = work[g : g + group].reshape(group * rows, 2 * m_count)
        o = product(z, table_high[...], table_low[...])
        for k in range(group):
            for c in range(2):
                block = o[k * rows : (k + 1) * rows, c * q_count : (c + 1) * q_count]
                begin = (g + k) * SUB
                turned = block.T
                for p, ref in enumerate(out):
                    ref[c, begin : begin + SUB, :] = turned[p * SUB : (p + 1) * SUB]


def middle_kernel(last, order, *refs):
    row_count = len(order)
    data = in_order(order, refs)
    turn, table_high, table_low, first_kernel, load, *rest = refs[row_count:]
    if last:
        second_kernel, older, *out, work = rest
    else:
        *out, kept, work = rest
    _, span, rows = data[0].shape

    def gather(t, carry):
        at = pl.ds(pl.multiple_of(t * SUB, SUB), SUB)
        zs = fft_list([(ref[0, at, :], ref[1, at, :]) for ref in data], -1.0)
        for k in range(row_count):
            c, s = turn[k, 0:1, :], turn[k, 1:2, :]
            work[k, at, :rows] = zs[k][0] * c + zs[k][1] * s
            work[k, at, rows:] = zs[k][1] * c - zs[k][0] * s
        return carry

    lax.fori_loop(0, span // SUB, gather, 0)
    group = group_of(row_count, span)
    for g in range(0, row_count, group):
        z = work[g : g + group].reshape(group * span, 2 * rows)
        spectrum = product(z, table_high[...], table_low[...]).reshape(group, span, 2 * rows)
        parts = (spectrum[:, :, :rows], spectrum[:, :, rows:])
        factor = first_kernel[g : g + group]
        loads = [load[c, g : g + group] + factor * parts[c] for c in range(2)]
        for c in range(2):
            if last:
                loads[c] = loads[c] + second_kernel[g : g + group] * older[c, g : g + group]
            else:
                kept[c, g : g + group] = parts[c]
        w = jnp.concatenate(loads, axis=2).reshape(group * span, 2 * rows)
        w = product(w, table_high[...], table_low[...], True)
        work[g : g + group] = w.reshape(group, span, 2 * rows)

    def scatter(t, carry):
        at = pl.ds(pl.multiple_of(t * SUB, SUB), SUB)
        zs = []
        for k in range(row_count):
            c, s = turn[k, 0:1, :], turn[k, 1:2, :]
            re, im = work[k, at, :rows], work[k, at, rows:]
            zs.append((re * c - im * s, im * c + re * s))
        zs = fft_list(zs, 1.0)
        for k in range(row_count):
            out[k][0, at, :] = zs[k][0]
            out[k][1, at, :] = zs[k][1]
        return carry

    lax.fori_loop(0, span // SUB, scatter, 0)


def inverse_y_kernel(n_count, order, *refs):
    data = in_order(order, refs)
    turn, table_high, table_low, own, other, work = refs[len(order) :]
    rows = data[0].shape[2]
    m_count = turn.shape[2]
    lane = lane_width(m_count)
    half = n_count // 2
    group = group_of(n_count, rows)
    for g in range(0, n_count, group):
        blocks = []
        for k in range(g, g + group):
            at = slice(k * SUB, (k + 1) * SUB)
            parts = [jnp.concatenate([ref[c, at, :] for ref in data], axis=0).T for c in range(2)]
            blocks.append(jnp.concatenate(parts, axis=1))
        z = jnp.concatenate(blocks, axis=0)
        o = product(z, table_high[...], table_low[...], True)
        work[g : g + group] = o.reshape(group, rows, 2 * m_count)

    def tile(t, carry):
        at = pl.ds(pl.multiple_of(t * SUB, SUB), SUB)
        for j in range(m_count // lane):
            ys = []
            for k in range(n_count):
                c = turn[k, 0:1, j * lane : (j + 1) * lane]
                s = turn[k, 1:2, j * lane : (j + 1) * lane]
                re = work[k, at, j * lane : (j + 1) * lane]
                im = work[k, at, m_count + j * lane : m_count + (j + 1) * lane]
                ys.append((re * c - im * s, im * c + re * s))
            ps = [(ys[0][0], None)]
            for k in range(1, half):
                both = cadd(ys[k], conj(ys[n_count - k]))
                ps.append((both[0] * 0.5, both[1] * 0.5))
            ps.append((ys[half][0], None))
            xs = irfft_list(ps)
            for n in range(half):
                begin = n * m_count + j * lane
                own[at, begin : begin + lane] = xs[n]
                other[at, begin : begin + lane] = xs[half + n]
        return carry

    lax.fori_loop(0, rows // SUB, tile, 0)


def load_kernel(fresh, kernel, history, loads, factor, sums, turned):
    horizon, block, length = kernel.shape
    step = pl.program_id(0)
    lane = lane_width(length)
    at = pl.ds(pl.multiple_of(step * block, block), block)

    def chunk(j, carry):
        cols = pl.ds(pl.multiple_of(j * lane, lane), lane)
        totals = [jnp.zeros((block, lane), f32) for _ in range(2)]
        for h in range(fresh, horizon):
            weight = kernel[h, :, cols].astype(f32)
            for c in range(2):
                totals[c] = totals[c] + weight * history[h - fresh, c, :, cols].astype(f32)
        for a, total in enumerate((*totals, kernel[fresh - 1, :, cols].astype(f32))):
            sums[a, j, at, :] = total
        return carry

    lax.fori_loop(0, length // lane, chunk, 0)

    @pl.when(step == pl.num_programs(0) - 1)
    def _():
        span = sums.shape[2]
        n_count = span // SUB
        row_count, _, rows = factor.shape
        for a, target in enumerate((loads.at[0], loads.at[1], factor)):
            for j in range(length // lane):
                pieces = [sums[a, j, pl.ds(k, SUB, stride=n_count), :] for k in range(n_count)]
                turned[j * lane : (j + 1) * lane, :span] = jnp.concatenate(pieces, axis=0).T
            for k in range(row_count):
                target[k] = turned[pl.ds(k, rows, stride=row_count), :][:, :span].T


def stencil_kernel(
    lower, upper, old_lower, old_upper, slip, cells, above, below, beside, base, strength, partial, following, grown
):
    rows, cols = slip.shape
    lane = beside.shape[2] // 2
    row_index = lax.broadcasted_iota(jnp.int32, (rows, cols), 0)
    col_index = lax.broadcasted_iota(jnp.int32, (rows, cols), 1)
    layers = ((lower, old_lower, upper, partial), (upper, old_upper, lower, following))
    for layer, (now, before, across, target) in enumerate(layers):
        here = now[0]
        up = pltpu.roll(here, 1, 0)
        up = jnp.where(row_index == 0, above[layer, SUB - 1 : SUB, :], up)
        down = pltpu.roll(here, rows - 1, 0)
        down = jnp.where(row_index == rows - 1, below[layer, 0:1, :], down)
        left = pltpu.roll(here, 1, 1)
        left = jnp.where(col_index == 0, beside[layer, :, 2 * lane - 1 : 2 * lane], left)
        right = pltpu.roll(here, cols - 1, 1)
        right = jnp.where(col_index == cols - 1, beside[layer, :, 0:1], right)
        flat = up + down + left + right - 4.0 * here
        normal = across[0] - 2.0 * here if layer else across[0] + here - 2.0 * here
        target[0] = 2.0 * here - before[0] + courant * (flat + normal)
    for r in range(cells.shape[1]):
        at = slice(r * BLOCK_CELLS, (r + 1) * BLOCK_CELLS)
        rate = lower[0, at, :] - old_lower[0, at, :]
        old = slip[at, :]
        base[at, :] = cells[3, r : r + 1, :] - damping * rate
        weak = jnp.minimum(old * cells[2, r : r + 1, :], 1.0)
        strength[at, :] = cells[0, r : r + 1, :] - cells[1, r : r + 1, :] * weak
        grown[at, :] = old + jnp.abs(rate)


def clipped(own, other, base, strength):
    limit = strength[...]
    return jnp.clip(base[...] + (own[...] + other[...]), -limit, limit)


def traction_kernel(own, other, base, strength, partial, current, following, rate):
    updated = partial[0] + courant * clipped(own, other, base, strength)
    following[0] = updated
    rate[...] = updated - current[0]


def last_traction_kernel(own, other, base, strength, partial, whole, following, result):
    traction = clipped(own, other, base, strength)
    result[...] = traction
    following[0] = partial[0] + courant * traction


def vmem():
    return pl.BlockSpec(memory_space=pltpu.VMEM)


def call(kernel, inputs, outputs, scratch=(), flops=0, name=None, limit=20 * 2**20):
    size = sum(int(np.prod(v.shape)) * v.dtype.itemsize for v in (*inputs, *outputs))
    return pl.pallas_call(
        kernel,
        in_specs=[vmem()] * len(inputs),
        out_specs=[vmem()] * len(outputs),
        out_shape=list(outputs),
        scratch_shapes=list(scratch),
        cost_estimate=pl.CostEstimate(flops=flops, transcendentals=0, bytes_accessed=size),
        name=name,
        compiler_params=pltpu.CompilerParams(vmem_limit_bytes=limit),
    )(*inputs)


def shards(
    wave_now,
    wave_before,
    fault_slip,
    region_ids,
    mode_history,
    wave_kernel,
    static_friction,
    dynamic_friction,
    weakening_slip,
    normal_stress,
    initial_stress,
):
    rows, cols = wave_now.shape[1], wave_now.shape[2]
    row_count = lax.axis_size("row")
    col_count = lax.axis_size("col")
    assert col_count == 2 and SUBSTEPS == 2
    width, length = cols * col_count, rows * row_count
    span = width // (row_count * col_count)
    n_count = span // SUB
    m_count = width // n_count
    horizon = mode_history.shape[0]
    row, col = lax.axis_index("row"), lax.axis_index("col")
    places = np.arange(row_count)[:, None] * (col_count * SUB) + np.arange(SUB)[None, :]
    table_y = table_of(m_count, places.reshape(-1))
    table_x = table_of(rows, np.arange(rows))

    def counts(first, second):
        shape = (first, second)
        return lax.broadcasted_iota(jnp.int32, shape, 0), lax.broadcasted_iota(jnp.int32, shape, 1)

    k, m = counts(n_count, m_count)
    block_start = span * (row * col_count + col)
    turn_y = phases(m * (k + block_start) + (width // 2) * (col * k), width, 1 / math.sqrt(width))
    k, i = counts(row_count, rows)
    turn_x = phases(k * (i + rows * row), length, 1 / math.sqrt(length))
    part_shape = jax.ShapeDtypeStruct((2, span, rows), f32)
    part_shapes = [part_shape] * row_count
    order = sorted(range(row_count), key=lambda p: (p > 0, -min(p, row_count - p), p))
    tile_shape = jax.ShapeDtypeStruct((rows, cols), f32)
    load_shape = jax.ShapeDtypeStruct((2, row_count, span, rows), f32)
    factor_shape = jax.ShapeDtypeStruct((row_count, span, rows), f32)

    def swap(value):
        return lax.ppermute(value, "col", [(0, 1), (1, 0)])

    def regroup(parts):
        if row_count > MAX_PERMUTES:
            whole = jnp.roll(jnp.stack(parts), row, axis=0)
            whole = lax.all_to_all(whole, "row", split_axis=0, concat_axis=0, tiled=True)
            whole = jnp.roll(whole, -row, axis=0)
            return [whole[place] for place in order]
        received = []
        for place in order:
            shift = -place % row_count
            pairs = [(i, (i + shift) % row_count) for i in range(row_count)]
            received.append(lax.ppermute(parts[shift], "row", pairs) if shift else parts[0])
        return received

    def cells_of(region_ids):
        chosen = region_ids[None] == jnp.arange(static_friction.shape[0], dtype=jnp.int32)[:, None, None]

        def lookup(table):
            return jnp.sum(jnp.where(chosen, table[:, None, None], 0.0), axis=0)

        normal_load = lookup(normal_stress)
        static_level = lookup(static_friction)
        blocks = jnp.stack(
            [
                normal_load * static_level,
                normal_load * (static_level - lookup(dynamic_friction)),
                1.0 / lookup(weakening_slip),
                lookup(initial_stress),
            ]
        )
        block_of = lax.broadcasted_iota(jnp.int32, (region_ids.shape[1], cols), 1) // BLOCK_CELLS
        spread = (block_of == lax.broadcasted_iota(jnp.int32, block_of.shape, 0)).astype(f32)
        return jnp.einsum("abc,cd->abd", blocks, spread, precision=lax.Precision.HIGHEST)

    def past_loads(fresh, wave_kernel, mode_history):
        block = 16
        return pl.pallas_call(
            functools.partial(load_kernel, fresh),
            grid=(span // block,),
            in_specs=[
                pl.BlockSpec((horizon, block, length), lambda b: (0, b, 0)),
                pl.BlockSpec((horizon - fresh, 2, block, length), lambda b: (0, 0, b, 0)),
            ],
            out_specs=[vmem()] * 2,
            out_shape=[load_shape, factor_shape],
            scratch_shapes=[
                pltpu.VMEM((3, length // lane_width(length), span, lane_width(length)), f32),
                pltpu.VMEM((length, max(span, LANES)), f32),
            ],
            cost_estimate=pl.CostEstimate(
                flops=20 * horizon * span * length, transcendentals=0, bytes_accessed=6 * horizon * span * length
            ),
            compiler_params=pltpu.CompilerParams(vmem_limit_bytes=50 * 2**20),
            name="past_loads",
        )(wave_kernel, mode_history)

    def forward(rate):
        work = pltpu.VMEM((n_count, rows, 2 * m_count), f32)
        inputs = (rate, swap(rate), turn_y, *table_y)
        kernel = functools.partial(forward_y_kernel, n_count)
        return call(kernel, inputs, part_shapes, [work], 10**9, "forward_y")

    def middle(last, data, *more):
        work = pltpu.VMEM((row_count, span, 2 * rows), f32)
        outputs = part_shapes if last else [*part_shapes, load_shape]
        inputs = (*data, turn_x, *table_x, *more)
        kernel = functools.partial(middle_kernel, last, order)
        return call(kernel, inputs, outputs, [work], 10**9, "middle")

    def inverse(data):
        work = pltpu.VMEM((n_count, rows, 2 * m_count), f32)
        kernel = functools.partial(inverse_y_kernel, n_count, order)
        inputs = (*data, turn_y, *table_y)
        own, other = call(kernel, inputs, [tile_shape] * 2, [work], 10**9, "inverse_y")
        return own, swap(other)

    ring = [(i, (i + 1) % row_count) for i in range(row_count)]
    edge = lane_width(cols)
    layer_shape = jax.ShapeDtypeStruct((1, rows, cols), f32)

    def halos(lower, upper):
        def edges(begin, size, axis):
            pick = lambda v: lax.slice_in_dim(v[0][v[1] : v[1] + 1], begin, begin + size, axis=axis)
            return jnp.concatenate([pick(lower), pick(upper)], axis=0)

        above = lax.ppermute(edges(rows - SUB, SUB, 1), "row", ring)
        below = lax.ppermute(edges(0, SUB, 1), "row", [(b, a) for a, b in ring])
        beside = swap(jnp.concatenate([edges(0, edge, 2), edges(cols - edge, edge, 2)], axis=2))
        return above, below, beside

    def stencil(last, cells, around, lower, upper, old_lower, old_upper, slip):
        layers = (lower, upper, old_lower, old_upper)
        more = (slip, cells, *around)

        def at_layer(index):
            return pl.BlockSpec((1, rows, cols), lambda i: (index, 0, 0))

        following = jax.ShapeDtypeStruct((2, rows, cols), f32) if last else layer_shape
        specs = [tile_shape, tile_shape, layer_shape, following, tile_shape]
        whole = pl.BlockSpec((rows, cols), lambda i: (0, 0))
        return pl.pallas_call(
            stencil_kernel,
            grid=(1,),
            in_specs=[at_layer(index) for _, index in layers] + [vmem()] * len(more),
            out_specs=[whole, whole, at_layer(0), at_layer(1 if last else 0), whole],
            out_shape=specs,
            cost_estimate=pl.CostEstimate(flops=5 * 10**9, transcendentals=0, bytes_accessed=40 * rows * cols),
            compiler_params=pltpu.CompilerParams(vmem_limit_bytes=40 * 2**20),
            name="stencil",
        )(*[v for v, _ in layers], *more)

    def traction_step(last, own, other, base, strength, partial, extra):
        step = 32 if rows % 32 == 0 else rows
        layer = pl.BlockSpec((1, step, cols), lambda i: (0, i, 0))
        tile = pl.BlockSpec((step, cols), lambda i: (i, 0))
        return pl.pallas_call(
            last_traction_kernel if last else traction_kernel,
            grid=(rows // step,),
            in_specs=[tile] * 4 + [layer, pl.BlockSpec(memory_space=pl.ANY) if last else layer],
            out_specs=[layer, tile],
            out_shape=[jax.ShapeDtypeStruct(extra.shape if last else (1, rows, cols), f32), tile_shape],
            input_output_aliases={5: 0} if last else {},
            compiler_params=pltpu.CompilerParams(vmem_limit_bytes=12 * 2**20),
            name="traction",
        )(own, other, base, strength, partial, extra)

    together = lax.optimization_barrier

    def meanwhile(parts, *work):
        parts, work = together((parts, work))
        return regroup(parts), work

    def after_first(data, work):
        first, work = together((data[1], work))
        return [data[0], first, *data[2:]], work

    parts = forward(wave_now[0] - wave_before[0])
    data, (kernel, history) = meanwhile(parts, wave_kernel, mode_history)
    data, now = after_first(data, wave_now)
    around = halos((now, 0), (now, 1))
    data, (load, first) = together((data, past_loads(1, kernel, history)))
    *parts, older = middle(False, data, first, load)
    data, (now, before, ids) = meanwhile(parts, wave_now, wave_before, region_ids)
    cells = cells_of(ids)
    found = stencil(False, cells, around, (now, 0), (now, 1), (before, 0), (before, 1), fault_slip)
    data, found = together((data, found))
    base, strength, partial, upper, slip = found
    own, other = inverse(data)
    lower, rate = traction_step(False, own, other, base, strength, partial, wave_now)

    parts = forward(rate)
    data, (kernel, history) = meanwhile(parts, wave_kernel, mode_history)
    data, (lower, upper) = after_first(data, (lower, upper))
    around = halos((lower, 0), (upper, 0))
    data, (load, second) = together((data, past_loads(2, kernel, history)))
    parts = middle(True, data, first, load, second, older)
    data, (lower, upper) = meanwhile(parts, lower, upper)
    found = stencil(True, cells, around, (lower, 0), (upper, 0), (wave_now, 0), (wave_now, 1), slip)
    data, found = together((data, found))
    base, strength, partial, following, slip = found
    own, other = inverse(data)
    current, traction = traction_step(True, own, other, base, strength, partial, following)
    return (current, slip, traction)


def solution(mesh):
    return jax.shard_map(
        shards,
        mesh=mesh,
        in_specs=(
            P("groups", "row", "col"),
            P("groups", "row", "col"),
            P(("groups", "row"), "col"),
            P(("groups", "row"), "col"),
            P("groups", None, ("row", "col"), None),
            P(None, ("row", "col"), None),
            P(),
            P(),
            P(),
            P(),
            P(),
        ),
        out_specs=(
            P("groups", "row", "col"),
            P(("groups", "row"), "col"),
            P(("groups", "row"), "col"),
        ),
        check_vma=False,
    )
```

```python
import functools
import math

import jax
import jax.numpy as jnp
import numpy as np
from jax import lax
from jax.experimental import pallas as pl
from jax.experimental.pallas import tpu as pltpu
from jax.sharding import PartitionSpec as P


SUBSTEPS = 2
BLOCK_CELLS = 16
LANES = 128
MAX_PERMUTES = 16
SUB = 8

damping = 0.5
courant = 0.3
f32 = jnp.float32
bf16 = jnp.bfloat16


def add(a, b):
    if a is None:
        return b
    return a if b is None else a + b


def sub(a, b):
    if b is None:
        return a
    return -b if a is None else a - b


def scale(z, w):
    re, im = z
    c, s = w.real, w.imag
    if abs(s) < 1e-12:
        return (re, im) if c > 0 else (-re, None if im is None else -im)
    if abs(c) < 1e-12:
        if s > 0:
            return (None if im is None else -im, re)
        return (im, None if re is None else -re)
    if im is None:
        return (re * c, re * s)
    if re is None:
        return (im * -s, im * c)
    if abs(abs(c) - abs(s)) < 1e-12:
        a = abs(c)
        signs = (c > 0, s > 0)
        if signs == (True, True):
            return ((re - im) * a, (re + im) * a)
        if signs == (True, False):
            return ((re + im) * a, (im - re) * a)
        if signs == (False, True):
            return ((re + im) * -a, (re - im) * a)
        return ((im - re) * a, (re + im) * -a)
    return (re * c - im * s, re * s + im * c)


def cadd(a, b):
    return (add(a[0], b[0]), add(a[1], b[1]))


def csub(a, b):
    return (sub(a[0], b[0]), sub(a[1], b[1]))


def conj(a):
    return (a[0], None if a[1] is None else -a[1])


def root(k, n, sign):
    return complex(math.cos(2 * math.pi * k / n), sign * math.sin(2 * math.pi * k / n))


def fft_list(zs, sign):
    n = len(zs)
    if n == 1:
        return list(zs)
    even = fft_list(zs[0::2], sign)
    odd = fft_list(zs[1::2], sign)
    low, high = [], []
    for k in range(n // 2):
        t = scale(odd[k], root(k, n, sign))
        low.append(cadd(even[k], t))
        high.append(csub(even[k], t))
    return low + high


def rfft_list(xs):
    n = len(xs)
    if n == 1:
        return [(xs[0], None)]
    if n == 2:
        return [(xs[0] + xs[1], None), (xs[0] - xs[1], None)]
    even = rfft_list(xs[0::2])
    odd = rfft_list(xs[1::2])
    out = [None] * (n // 2 + 1)
    for k in range(n // 4 + 1):
        t = scale(odd[k], root(k, n, -1.0))
        out[k] = cadd(even[k], t)
        if n // 2 - k != k:
            out[n // 2 - k] = conj(csub(even[k], t))
    return out


def irfft_list(ps):
    n = 2 * (len(ps) - 1)
    if n == 2:
        return [ps[0][0] + ps[1][0], ps[0][0] - ps[1][0]]
    even, odd = [], []
    for k in range(n // 4 + 1):
        mirrored = conj(ps[n // 2 - k])
        even.append(cadd(ps[k], mirrored))
        odd.append(scale(csub(ps[k], mirrored), root(k, n, 1.0)))
    a, b = irfft_list(even), irfft_list(odd)
    return [v for pair in zip(a, b) for v in pair]


def halves(table):
    high = table.astype(np.float32).astype(bf16)
    low = (table - high.astype(np.float64)).astype(np.float32).astype(bf16)
    return jnp.asarray(high), jnp.asarray(low)


def complex_block(re, im):
    return np.block([[re, im], [-im, re]])


def table_of(count, picked):
    angle = 2 * np.pi * np.outer(np.arange(count), picked) / count
    return halves(complex_block(np.cos(angle), -np.sin(angle)))


def phases(index, period, norm):
    angle = (index % period).astype(f32) * (2 * math.pi / period)
    return jnp.stack([jnp.cos(angle), jnp.sin(angle)], axis=1) * norm


def split(z):
    high = z.astype(bf16)
    return high, (z - high.astype(f32)).astype(bf16)


def product(z, table_high, table_low, inverse=False):
    high, low = split(z)

    def dot(a, b):
        return lax.dot_general(a, b, (((1,), (1 if inverse else 0,)), ((), ())), preferred_element_type=f32)

    return dot(high, table_high) + dot(low, table_high) + dot(high, table_low)


def group_of(count, rows):
    group = count
    while group > 1 and group * rows > 512:
        group //= 2
    return group


def in_order(order, refs):
    placed = [None] * len(order)
    for place, ref in zip(order, refs):
        placed[place] = ref
    return placed


def lane_width(count):
    return min(LANES, count)


def halo_places(part, cols, layer):
    _, span, width = part.shape
    count = cols // width
    places = [divmod(t, span) for t in range(layer * count, (layer + 1) * count)]
    return [(2 + slab, slice(row, row + 1)) for slab, row in places]


def forward_y_kernel(n_count, edges, own, other, turn, table_high, table_low, *rest):
    sources, (*out, work) = rest[:2], rest[2:]
    rows = own.shape[0]
    m_count = turn.shape[2]
    lane = lane_width(m_count)
    half = n_count // 2

    def tile(t, carry):
        at = pl.ds(pl.multiple_of(t * SUB, SUB), SUB)
        for j in range(m_count // lane):
            xs = []
            for ref in (own, other):
                for n in range(half):
                    begin = n * m_count + j * lane
                    xs.append(ref[at, begin : begin + lane])
            spectrum = rfft_list(xs)
            for k in range(n_count):
                z = spectrum[k] if k <= half else conj(spectrum[n_count - k])
                c = turn[k, 0:1, j * lane : (j + 1) * lane]
                s = turn[k, 1:2, j * lane : (j + 1) * lane]
                if z[1] is None:
                    re, im = z[0] * c, z[0] * -s
                else:
                    re, im = z[0] * c + z[1] * s, z[1] * c - z[0] * s
                work[k, at, j * lane : (j + 1) * lane] = re
                work[k, at, m_count + j * lane : m_count + (j + 1) * lane] = im
        return carry

    lax.fori_loop(0, rows // SUB, tile, 0)
    group = group_of(n_count, rows)
    q_count = len(out) * SUB
    for g in range(0, n_count, group):
        z = work[g : g + group].reshape(group * rows, 2 * m_count)
        o = product(z, table_high[...], table_low[...])
        for k in range(group):
            for c in range(2):
                block = o[k * rows : (k + 1) * rows, c * q_count : (c + 1) * q_count]
                begin = (g + k) * SUB
                turned = block.T
                for p, ref in enumerate(out):
                    ref[c, begin : begin + SUB, :] = turned[p * SUB : (p + 1) * SUB]
    for ref, picks in zip((out[1], out[-1]), edges):
        for layer, (source, index, row) in enumerate(picks):
            for j, (slab, at) in enumerate(halo_places(ref, sources[source].shape[2], layer)):
                ref[slab, at, :] = sources[source][index, row : row + 1, j * rows : (j + 1) * rows]


def middle_kernel(last, order, *refs):
    row_count = len(order)
    data = in_order(order, refs)
    turn, table_high, table_low, first_kernel, load, *rest = refs[row_count:]
    if last:
        second_kernel, older, *out, work = rest
    else:
        *out, kept, work = rest
    _, span, rows = data[0].shape

    def gather(t, carry):
        at = pl.ds(pl.multiple_of(t * SUB, SUB), SUB)
        zs = fft_list([(ref[0, at, :], ref[1, at, :]) for ref in data], -1.0)
        for k in range(row_count):
            c, s = turn[k, 0:1, :], turn[k, 1:2, :]
            work[k, at, :rows] = zs[k][0] * c + zs[k][1] * s
            work[k, at, rows:] = zs[k][1] * c - zs[k][0] * s
        return carry

    lax.fori_loop(0, span // SUB, gather, 0)
    group = group_of(row_count, span)
    for g in range(0, row_count, group):
        z = work[g : g + group].reshape(group * span, 2 * rows)
        spectrum = product(z, table_high[...], table_low[...]).reshape(group, span, 2 * rows)
        parts = (spectrum[:, :, :rows], spectrum[:, :, rows:])
        factor = first_kernel[g : g + group]
        loads = [load[c, g : g + group] + factor * parts[c] for c in range(2)]
        for c in range(2):
            if last:
                loads[c] = loads[c] + second_kernel[g : g + group] * older[c, g : g + group]
            else:
                kept[c, g : g + group] = parts[c]
        w = jnp.concatenate(loads, axis=2).reshape(group * span, 2 * rows)
        w = product(w, table_high[...], table_low[...], True)
        work[g : g + group] = w.reshape(group, span, 2 * rows)

    def scatter(t, carry):
        at = pl.ds(pl.multiple_of(t * SUB, SUB), SUB)
        zs = []
        for k in range(row_count):
            c, s = turn[k, 0:1, :], turn[k, 1:2, :]
            re, im = work[k, at, :rows], work[k, at, rows:]
            zs.append((re * c - im * s, im * c + re * s))
        zs = fft_list(zs, 1.0)
        for k in range(row_count):
            out[k][0, at, :] = zs[k][0]
            out[k][1, at, :] = zs[k][1]
        return carry

    lax.fori_loop(0, span // SUB, scatter, 0)


def inverse_y_kernel(n_count, order, *refs):
    data = in_order(order, refs)
    turn, table_high, table_low, own, other, work = refs[len(order) :]
    rows = data[0].shape[2]
    m_count = turn.shape[2]
    lane = lane_width(m_count)
    half = n_count // 2
    group = group_of(n_count, rows)
    for g in range(0, n_count, group):
        blocks = []
        for k in range(g, g + group):
            at = slice(k * SUB, (k + 1) * SUB)
            parts = [jnp.concatenate([ref[c, at, :] for ref in data], axis=0).T for c in range(2)]
            blocks.append(jnp.concatenate(parts, axis=1))
        z = jnp.concatenate(blocks, axis=0)
        o = product(z, table_high[...], table_low[...], True)
        work[g : g + group] = o.reshape(group, rows, 2 * m_count)

    def tile(t, carry):
        at = pl.ds(pl.multiple_of(t * SUB, SUB), SUB)
        for j in range(m_count // lane):
            ys = []
            for k in range(n_count):
                c = turn[k, 0:1, j * lane : (j + 1) * lane]
                s = turn[k, 1:2, j * lane : (j + 1) * lane]
                re = work[k, at, j * lane : (j + 1) * lane]
                im = work[k, at, m_count + j * lane : m_count + (j + 1) * lane]
                ys.append((re * c - im * s, im * c + re * s))
            ps = [(ys[0][0], None)]
            for k in range(1, half):
                both = cadd(ys[k], conj(ys[n_count - k]))
                ps.append((both[0] * 0.5, both[1] * 0.5))
            ps.append((ys[half][0], None))
            xs = irfft_list(ps)
            for n in range(half):
                begin = n * m_count + j * lane
                own[at, begin : begin + lane] = xs[n]
                other[at, begin : begin + lane] = xs[half + n]
        return carry

    lax.fori_loop(0, rows // SUB, tile, 0)


def load_kernel(fresh, kernel, history, loads, factor, sums, turned):
    horizon, block, length = kernel.shape
    step = pl.program_id(0)
    lane = lane_width(length)
    at = pl.ds(pl.multiple_of(step * block, block), block)

    def chunk(j, carry):
        cols = pl.ds(pl.multiple_of(j * lane, lane), lane)
        totals = [jnp.zeros((block, lane), f32) for _ in range(2)]
        for h in range(fresh, horizon):
            weight = kernel[h, :, cols].astype(f32)
            for c in range(2):
                totals[c] = totals[c] + weight * history[h - fresh, c, :, cols].astype(f32)
        for a, total in enumerate((*totals, kernel[fresh - 1, :, cols].astype(f32))):
            sums[a, j, at, :] = total
        return carry

    lax.fori_loop(0, length // lane, chunk, 0)

    @pl.when(step == pl.num_programs(0) - 1)
    def _():
        span = sums.shape[2]
        n_count = span // SUB
        row_count, _, rows = factor.shape
        for a, target in enumerate((loads.at[0], loads.at[1], factor)):
            for j in range(length // lane):
                pieces = [sums[a, j, pl.ds(k, SUB, stride=n_count), :] for k in range(n_count)]
                turned[j * lane : (j + 1) * lane, :span] = jnp.concatenate(pieces, axis=0).T
            for k in range(row_count):
                target[k] = turned[pl.ds(k, rows, stride=row_count), :][:, :span].T


def stencil_kernel(
    columns, lower, upper, old_lower, old_upper, slip, cells, above, below, beside, base, strength, partial, following, grown
):
    rows, cols = slip.shape

    def halo_row(part, layer):
        return jnp.concatenate([part[slab, at, :] for slab, at in halo_places(part, cols, layer)], axis=1)

    def halo_column(index):
        return beside[:, columns[index] : columns[index] + 1]

    row_index = lax.broadcasted_iota(jnp.int32, (rows, cols), 0)
    col_index = lax.broadcasted_iota(jnp.int32, (rows, cols), 1)
    layers = ((lower, old_lower, upper, partial), (upper, old_upper, lower, following))
    for layer, (now, before, across, target) in enumerate(layers):
        here = now[0]
        up = pltpu.roll(here, 1, 0)
        up = jnp.where(row_index == 0, halo_row(above, layer), up)
        down = pltpu.roll(here, rows - 1, 0)
        down = jnp.where(row_index == rows - 1, halo_row(below, layer), down)
        left = pltpu.roll(here, 1, 1)
        left = jnp.where(col_index == 0, halo_column(2 * layer + 1), left)
        right = pltpu.roll(here, cols - 1, 1)
        right = jnp.where(col_index == cols - 1, halo_column(2 * layer), right)
        flat = up + down + left + right - 4.0 * here
        normal = across[0] - 2.0 * here if layer else across[0] + here - 2.0 * here
        target[0] = 2.0 * here - before[0] + courant * (flat + normal)
    for r in range(cells.shape[1]):
        at = slice(r * BLOCK_CELLS, (r + 1) * BLOCK_CELLS)
        rate = lower[0, at, :] - old_lower[0, at, :]
        old = slip[at, :]
        base[at, :] = cells[3, r : r + 1, :] - damping * rate
        weak = jnp.minimum(old * cells[2, r : r + 1, :], 1.0)
        strength[at, :] = cells[0, r : r + 1, :] - cells[1, r : r + 1, :] * weak
        grown[at, :] = old + jnp.abs(rate)


def clipped(own, other, base, strength):
    limit = strength[...]
    return jnp.clip(base[...] + (own[...] + other[...]), -limit, limit)


def put_rate(rate, lower, upper, old_lower):
    rows, cols = lower.shape
    rate[:, :cols] = lower - old_lower
    lane = lax.broadcasted_iota(jnp.int32, (rows, LANES), 1)
    columns = [v[:, c : c + 1] for v in (lower, upper) for c in (0, cols - 1)]
    packed = columns[3]
    for index in range(3):
        packed = jnp.where(lane == index, columns[index], packed)
    rate[:, cols:] = jnp.broadcast_to(packed, (rows, LANES))


def traction_kernel(own, other, base, strength, partial, current, upper, following, rate):
    updated = partial[0] + courant * clipped(own, other, base, strength)
    following[0] = updated
    put_rate(rate, updated, upper[0], current[0])


def last_traction_kernel(own, other, base, strength, partial, whole, following, result):
    traction = clipped(own, other, base, strength)
    result[...] = traction
    following[0] = partial[0] + courant * traction


def vmem():
    return pl.BlockSpec(memory_space=pltpu.VMEM)


def call(kernel, inputs, outputs, scratch=(), flops=0, limit=20 * 2**20):
    size = sum(int(np.prod(v.shape)) * v.dtype.itemsize for v in (*inputs, *outputs))
    return pl.pallas_call(
        kernel,
        in_specs=[vmem()] * len(inputs),
        out_specs=[vmem()] * len(outputs),
        out_shape=list(outputs),
        scratch_shapes=list(scratch),
        cost_estimate=pl.CostEstimate(flops=flops, transcendentals=0, bytes_accessed=size),
        compiler_params=pltpu.CompilerParams(vmem_limit_bytes=limit),
    )(*inputs)


def shards(
    wave_now,
    wave_before,
    fault_slip,
    region_ids,
    mode_history,
    wave_kernel,
    static_friction,
    dynamic_friction,
    weakening_slip,
    normal_stress,
    initial_stress,
):
    rows, cols = wave_now.shape[1], wave_now.shape[2]
    row_count = lax.axis_size("row")
    col_count = lax.axis_size("col")
    assert col_count == 2 and SUBSTEPS == 2
    width, length = cols * col_count, rows * row_count
    span = width // (row_count * col_count)
    n_count = span // SUB
    m_count = width // n_count
    horizon = mode_history.shape[0]
    row, col = lax.axis_index("row"), lax.axis_index("col")
    places = np.arange(row_count)[:, None] * (col_count * SUB) + np.arange(SUB)[None, :]
    table_y = table_of(m_count, places.reshape(-1))
    table_x = table_of(rows, np.arange(rows))

    def counts(first, second):
        shape = (first, second)
        return lax.broadcasted_iota(jnp.int32, shape, 0), lax.broadcasted_iota(jnp.int32, shape, 1)

    k, m = counts(n_count, m_count)
    block_start = span * (row * col_count + col)
    turn_y = phases(m * (k + block_start) + (width // 2) * (col * k), width, 1 / math.sqrt(width))
    k, i = counts(row_count, rows)
    turn_x = phases(k * (i + rows * row), length, 1 / math.sqrt(length))
    part_shape = jax.ShapeDtypeStruct((2, span, rows), f32)
    part_shapes = [part_shape] * row_count
    slabs = -(-2 * (cols // rows) // span)
    edge_shape = jax.ShapeDtypeStruct((2 + slabs, span, rows), f32)
    edged_shapes = [edge_shape if p in (1, row_count - 1) else part_shape for p in range(row_count)]
    rate_shape = jax.ShapeDtypeStruct((rows, cols + LANES), f32)
    order = sorted(range(row_count), key=lambda p: (p > 0, -min(p, row_count - p), p))
    tile_shape = jax.ShapeDtypeStruct((rows, cols), f32)
    load_shape = jax.ShapeDtypeStruct((2, row_count, span, rows), f32)
    factor_shape = jax.ShapeDtypeStruct((row_count, span, rows), f32)

    def swap(value):
        return lax.ppermute(value, "col", [(0, 1), (1, 0)])

    def regroup(parts):
        if row_count > MAX_PERMUTES:
            whole = jnp.roll(jnp.stack([v[:2] for v in parts]), row, axis=0)
            whole = lax.all_to_all(whole, "row", split_axis=0, concat_axis=0, tiled=True)
            whole = list(jnp.roll(whole, -row, axis=0))
            if parts[1].shape[0] > 2:
                for shift in (1, row_count - 1):
                    pairs = [(i, (i + shift) % row_count) for i in range(row_count)]
                    more = lax.ppermute(parts[shift][2:], "row", pairs)
                    whole[-shift] = jnp.concatenate([whole[-shift], more], axis=0)
            return [whole[place] for place in order]
        received = []
        for place in order:
            shift = -place % row_count
            pairs = [(i, (i + shift) % row_count) for i in range(row_count)]
            received.append(lax.ppermute(parts[shift], "row", pairs) if shift else parts[0])
        return received

    def cells_of(region_ids):
        chosen = region_ids[None] == jnp.arange(static_friction.shape[0], dtype=jnp.int32)[:, None, None]

        def lookup(table):
            return jnp.sum(jnp.where(chosen, table[:, None, None], 0.0), axis=0)

        normal_load = lookup(normal_stress)
        static_level = lookup(static_friction)
        blocks = jnp.stack(
            [
                normal_load * static_level,
                normal_load * (static_level - lookup(dynamic_friction)),
                1.0 / lookup(weakening_slip),
                lookup(initial_stress),
            ]
        )
        block_of = lax.broadcasted_iota(jnp.int32, (region_ids.shape[1], cols), 1) // BLOCK_CELLS
        spread = (block_of == lax.broadcasted_iota(jnp.int32, block_of.shape, 0)).astype(f32)
        return jnp.einsum("abc,cd->abd", blocks, spread, precision=lax.Precision.HIGHEST)

    def past_loads(fresh, wave_kernel, mode_history):
        block = 16
        return pl.pallas_call(
            functools.partial(load_kernel, fresh),
            grid=(span // block,),
            in_specs=[
                pl.BlockSpec((horizon, block, length), lambda b: (0, b, 0)),
                pl.BlockSpec((horizon - fresh, 2, block, length), lambda b: (0, 0, b, 0)),
            ],
            out_specs=[vmem()] * 2,
            out_shape=[load_shape, factor_shape],
            scratch_shapes=[
                pltpu.VMEM((3, length // lane_width(length), span, lane_width(length)), f32),
                pltpu.VMEM((length, max(span, LANES)), f32),
            ],
            cost_estimate=pl.CostEstimate(
                flops=20 * horizon * span * length, transcendentals=0, bytes_accessed=6 * horizon * span * length
            ),
            compiler_params=pltpu.CompilerParams(vmem_limit_bytes=46 * 2**20),
            name="past_loads",
        )(wave_kernel, mode_history)

    def forward(rate, other, edges, *sources):
        work = pltpu.VMEM((n_count, rows, 2 * m_count), f32)
        inputs = (rate, other, turn_y, *table_y, *sources)
        kernel = functools.partial(forward_y_kernel, n_count, edges)
        return call(kernel, inputs, edged_shapes, [work], 10**9)

    def middle(last, data, *more):
        work = pltpu.VMEM((row_count, span, 2 * rows), f32)
        outputs = part_shapes if last else [*part_shapes, load_shape]
        inputs = (*data, turn_x, *table_x, *more)
        kernel = functools.partial(middle_kernel, last, order)
        return call(kernel, inputs, outputs, [work], 10**9)

    def inverse(data):
        work = pltpu.VMEM((n_count, rows, 2 * m_count), f32)
        kernel = functools.partial(inverse_y_kernel, n_count, order)
        inputs = (*data, turn_y, *table_y)
        own, other = call(kernel, inputs, [tile_shape] * 2, [work], 10**9)
        return own, swap(other)

    layer_shape = jax.ShapeDtypeStruct((1, rows, cols), f32)

    def stencil(last, columns, cells, around, lower, upper, old_lower, old_upper, slip):
        layers = (lower, upper, old_lower, old_upper)
        more = (slip, cells, *around)

        def at_layer(index):
            return pl.BlockSpec((1, rows, cols), lambda i: (index, 0, 0))

        following = jax.ShapeDtypeStruct((2, rows, cols), f32) if last else layer_shape
        specs = [tile_shape, tile_shape, layer_shape, following, tile_shape]
        whole = pl.BlockSpec((rows, cols), lambda i: (0, 0))
        return pl.pallas_call(
            functools.partial(stencil_kernel, columns),
            grid=(1,),
            in_specs=[at_layer(index) for _, index in layers] + [vmem()] * len(more),
            out_specs=[whole, whole, at_layer(0), at_layer(1 if last else 0), whole],
            out_shape=specs,
            cost_estimate=pl.CostEstimate(flops=5 * 10**9, transcendentals=0, bytes_accessed=40 * rows * cols),
            compiler_params=pltpu.CompilerParams(vmem_limit_bytes=40 * 2**20),
            name="stencil",
        )(*[v for v, _ in layers], *more)

    def by_rows(kernel, inputs, outputs, aliases={}, limit=12 * 2**20):
        step = 32 if rows % 32 == 0 else rows

        def band(v):
            if len(v.shape) == 2:
                return pl.BlockSpec((step, v.shape[1]), lambda i: (i, 0))
            return pl.BlockSpec((v.shape[0], step, cols), lambda i: (0, i, 0))

        layer = pl.BlockSpec((1, step, cols), lambda i: (0, i, 0))
        return pl.pallas_call(
            kernel,
            grid=(rows // step,),
            in_specs=[
                pl.BlockSpec(memory_space=pl.ANY) if i in aliases else layer if isinstance(v, tuple) else band(v)
                for i, v in enumerate(inputs)
            ],
            out_specs=[layer if len(v.shape) == 3 else band(v) for v in outputs],
            out_shape=list(outputs),
            input_output_aliases=aliases,
            compiler_params=pltpu.CompilerParams(vmem_limit_bytes=limit),
        )(*[v[0] if isinstance(v, tuple) else v for v in inputs])

    together = lax.optimization_barrier

    def meanwhile(parts, *work):
        parts, work = together((parts, work))
        return regroup(parts), work

    def neighbours(data):
        return [data[order.index(place)] for place in (row_count - 1, 1)]

    rate = wave_now[0] - wave_before[0]
    tops, bottoms = wave_now[:, :SUB], wave_now[:, rows - SUB :]
    edges = ([(1, 0, SUB - 1), (1, 1, SUB - 1)], [(0, 0, 0), (0, 1, 0)])
    parts = forward(rate, swap(rate), edges, tops, bottoms)
    data, (kernel, history) = meanwhile(parts, wave_kernel, mode_history)
    data, (load, first) = together((data, past_loads(1, kernel, history)))
    around = neighbours(data)
    *parts, older = middle(False, data, first, load)
    data, (now, before, ids) = meanwhile(parts, wave_now, wave_before, region_ids)
    first_come, edge_of = together((data[1], now))
    data = [data[0], first_come, *data[2:]]
    lane = lane_width(cols)
    both = jnp.concatenate([edge_of[:, :, :lane], edge_of[:, :, cols - lane :]], axis=2)
    beside = swap(jnp.concatenate([both[0], both[1]], axis=1))
    columns = [0, 2 * lane - 1, 2 * lane, 4 * lane - 1]
    cells = cells_of(ids)
    around = (*around, beside)
    found = stencil(False, columns, cells, around, (now, 0), (now, 1), (before, 0), (before, 1), fault_slip)
    data, found = together((data, found))
    base, strength, partial, upper, slip = found
    own, other = inverse(data)
    inputs = (own, other, base, strength, partial, (wave_now,), upper)
    lower, rate = by_rows(traction_kernel, inputs, [layer_shape, rate_shape])

    beside = swap(rate)
    columns = [cols, cols + 1, cols + 2, cols + 3]
    edges = ([(0, 0, rows - 1), (1, 0, rows - 1)], [(0, 0, 0), (1, 0, 0)])
    parts = forward(rate, beside, edges, lower, upper)
    data, (kernel, history) = meanwhile(parts, wave_kernel, mode_history)
    data, (load, second) = together((data, past_loads(2, kernel, history)))
    around = (*neighbours(data), beside)
    parts = middle(True, data, first, load, second, older)
    data, (lower, upper) = meanwhile(parts, lower, upper)
    layers = ((lower, 0), (upper, 0), (wave_now, 0), (wave_now, 1))
    found = stencil(True, columns, cells, around, *layers, slip)
    data, found = together((data, found))
    base, strength, partial, following, slip = found
    own, other = inverse(data)
    inputs = (own, other, base, strength, partial, following)
    outputs = [jax.ShapeDtypeStruct(following.shape, f32), tile_shape]
    current, traction = by_rows(last_traction_kernel, inputs, outputs, {5: 0})
    return (current, slip, traction)


def solution(mesh):
    return jax.shard_map(
        shards,
        mesh=mesh,
        in_specs=(
            P("groups", "row", "col"),
            P("groups", "row", "col"),
            P(("groups", "row"), "col"),
            P(("groups", "row"), "col"),
            P("groups", None, ("row", "col"), None),
            P(None, ("row", "col"), None),
            P(),
            P(),
            P(),
            P(),
            P(),
        ),
        out_specs=(
            P("groups", "row", "col"),
            P(("groups", "row"), "col"),
            P(("groups", "row"), "col"),
        ),
        check_vma=False,
    )
```
